1024 devices in a mesh: mem: 32 (over y_hi, x), strip: 32 (over z, y_lo, core).
Axes of the slice: x: 8, y: 8 (y_hi: 4, y_lo: 2; y = y_hi * 2 + y_lo), z: 8, core: 2. Of those that a mesh axis runs over, the one named last changes fastest.
Arguments:
- ensemble: float32 [256, 256, 2048], P('mem', 'strip'), may hold values from -12 to 12
- forcing: float32 [256, 2048], P('strip'), may hold values from 4 to 12
- obs_index: int32 [2048, 128], P(('strip', 'mem')), may hold values from 0 to 255
- obs_count: int32 [2048], P(('strip', 'mem')), may hold values from 1 to 128, as said below
- obs_value: float32 [2048, 128], P(('strip', 'mem')), may hold values from -18 to 18
- obs_precision: float32 [2048, 128], P(('strip', 'mem')), may hold values from 0.05 to 1
Outputs:
- analysis: float32 [256, 256, 2048], P('mem', 'strip')
The draws below stay inside these ranges and needn't reach their ends.
Inputs may be any that keep to these rules, and one draw needn't show every extreme that they name: The live observations of a region are the first obs_count of its slots; in every draw some region has all 128 slots live. `obs_index`: position of the observed cell within its region; a cell may be observed more than once.
All inputs are finite; a program needn't handle non-finite values.
Results may differ from the reference program's by a relative error of at most 0.0003.
Values sent between devices are 32-bit elements; how exact they have to be, the bound alone decides.
No kernel may reach another device: no remote copies, remote signals or barrier semaphores. Data moves between devices by JAX's collectives and lax.ppermute only.
A program may use at most 32 MiB of HBM per device.

```python
import math
import jax
import jax.numpy as jnp
from jax import lax

MEMBER_TOTAL = 256
STEPS = 4
NS_ITERS = 4
REGION_VALUES = 256
OBS_MAX = 128
NLAT = 256
LON = 2048
REGION_TOTAL = 2048


def draw_obs_count(key, part):
    key_counts, key_chosen = jax.random.split(jax.random.fold_in(key, 11))
    counts = jax.random.randint(key_counts, (REGION_TOTAL,), 1, OBS_MAX + 1, dtype=jnp.int32)
    chosen = jax.random.randint(key_chosen, (), 0, REGION_TOTAL, dtype=jnp.int32)
    return jnp.where(jnp.arange(REGION_TOTAL, dtype=jnp.int32) == chosen, jnp.int32(OBS_MAX), counts)


def place_ends(values, key, smallest, high):
    extent = values.shape
    place = [jax.random.randint(jax.random.fold_in(key, axis), (), 0, extent[axis]) for axis in range(len(extent))]
    values = values.at[tuple(place)].set(smallest)
    longest = extent.index(max(extent))
    place[longest] = (place[longest] + 1) % extent[longest]
    return values.at[tuple(place)].set(high)


def level_of(own_key, dims, pieces, smallest, high):
    gain, own = 1.0, jax.random.fold_in(own_key, 6)
    for axis_at, parts in pieces:
        heights = jnp.exp(jax.random.uniform(jax.random.fold_in(own, axis_at), (parts,), jnp.float32, smallest / len(pieces), high / len(pieces)))
        gain = gain * jnp.repeat(heights, dims[axis_at] // parts).reshape([-1 if axis == axis_at else 1 for axis in range(len(dims))])
    return gain


def noise(key, extent, deviation, most, pieces=(), held_as=jnp.bfloat16):
    gain = level_of(key, extent, pieces, -0.22, 0.18) if pieces else 1.0
    values = jax.random.normal(key, extent, jnp.float32) * deviation * gain
    return jnp.minimum(jnp.maximum(values, -most), most).astype(held_as)


def setup_inputs(seed: int = 0) -> dict:
    keys = jax.random.split(jax.random.key(seed), 7)
    return {
        "ensemble": noise(keys[0], (MEMBER_TOTAL, NLAT, LON), 2.0, 12.0, ((0, 32), (1, 32)), jnp.float32),
        "forcing": jnp.clip(4.0 + 8.0 * jax.random.uniform(keys[1], (NLAT, LON), jnp.float32) ** level_of(keys[1], (NLAT, LON), ((0, 32),), -0.2, 0.2), 4.0, 12.0),
        "obs_index": place_ends(jax.random.randint(keys[2], (REGION_TOTAL, OBS_MAX), 0, REGION_VALUES), jax.random.fold_in(keys[2], 1), 0, REGION_VALUES - 1).astype(jnp.int32),
        "obs_count": draw_obs_count(jax.random.fold_in(keys[6], 71), 0),
        "obs_value": noise(keys[4], (REGION_TOTAL, OBS_MAX), 3.0, 18.0, ((0, 1024),), jnp.float32),
        "obs_precision": jnp.clip(jnp.exp(math.log(1.0) - 2.9957323 * jax.random.uniform(keys[5], (REGION_TOTAL, OBS_MAX), jnp.float32) ** level_of(keys[5], (REGION_TOTAL, OBS_MAX), ((0, 1024),), -0.2, 0.2)), 0.05, 1.0),
    }


step_size = 0.05
coupling = 0.4

def predict_increment(present_state, forcing):
    zero_row = jnp.zeros((1, present_state.shape[1]), present_state.dtype)
    padded_state = jnp.concatenate([zero_row, present_state, zero_row], axis=0)
    meridional = padded_state[2:] + padded_state[:-2] - 2.0 * present_state
    advection = (jnp.roll(present_state, -1, 1) - jnp.roll(present_state, 2, 1)) * jnp.roll(present_state, 1, 1)
    return present_state + step_size * (advection - present_state + forcing) + coupling * meridional

def analyze(members, obs_index, obs_count, obs_value, obs_precision):
    highest = lax.Precision.HIGHEST
    ens_size = members.shape[0]
    member_mean = lax.optimization_barrier(jnp.mean(members, axis=0))
    spread = members - member_mean[None]
    cell_ids = jnp.arange(members.shape[2], dtype=jnp.int32)
    onehot = (obs_index[:, :, None] == cell_ids[None, None, :]).astype(jnp.float32)
    slot_ids = jnp.arange(obs_index.shape[1], dtype=jnp.int32)
    live_mask = (slot_ids[None, :] < obs_count[:, None]).astype(jnp.float32)
    obs_spread = jnp.einsum('roc,krc->rok', onehot, spread, precision=highest)
    obs_mean = jnp.einsum('roc,rc->ro', onehot, member_mean, precision=highest)
    weight = obs_precision * live_mask
    innovation = weight * (obs_value - obs_mean)
    gram_matrix = jnp.einsum('roj,rok->rjk', obs_spread * weight[:, :, None], obs_spread, precision=highest)
    identity = jnp.eye(ens_size, dtype=jnp.float32)
    norm_scale = ens_size - 1.0 + jnp.sqrt(lax.optimization_barrier(jnp.sum(gram_matrix * gram_matrix, axis=(1, 2))))
    left_iterate = ((ens_size - 1.0) * identity + gram_matrix) / norm_scale[:, None, None]
    right_iterate = jnp.broadcast_to(identity, gram_matrix.shape)
    for repeat in range(NS_ITERS):
        correction = 1.5 * identity - 0.5 * jnp.einsum('rij,rjk->rik', right_iterate, left_iterate, precision=highest)
        left_iterate = jnp.einsum('rij,rjk->rik', left_iterate, correction, precision=highest)
        right_iterate = jnp.einsum('rij,rjk->rik', correction, right_iterate, precision=highest)
    inv_root = right_iterate / jnp.sqrt(norm_scale)[:, None, None]
    projected = jnp.einsum('roj,ro->rj', obs_spread, innovation, precision=highest)
    halfway = jnp.einsum('rjk,rk->rj', inv_root, projected, precision=highest)
    mean_weights = jnp.einsum('rjk,rk->rj', inv_root, halfway, precision=highest)
    transform = math.sqrt(ens_size - 1.0) * inv_root + mean_weights[:, :, None]
    return member_mean[None] + jnp.einsum('rjk,jrc->krc', transform, spread, precision=highest)

def reference(ensemble, forcing, obs_index, obs_count, obs_value, obs_precision):

    def integrate_model(member_state):
        for repeat in range(STEPS):
            member_state = predict_increment(member_state, forcing)
        return member_state
    predicted_state = lax.map(integrate_model, ensemble)
    region_blocks = predicted_state.reshape(MEMBER_TOTAL, REGION_TOTAL, REGION_VALUES).transpose(1, 0, 2)

    def solve_region(packed):
        members, index_row, count_one, value_row, precision_row = packed
        result = analyze(members[:, None, :], index_row[None], count_one[None], value_row[None], precision_row[None])
        return result[:, 0, :]
    analysis = lax.map(solve_region, (region_blocks, obs_index, obs_count, obs_value, obs_precision))
    return analysis.transpose(1, 0, 2).reshape(MEMBER_TOTAL, NLAT, LON)
```

```python
import functools
import math

import jax
import jax.numpy as jnp
from jax import lax
from jax.experimental import pallas as pl
from jax.experimental.pallas import tpu as pltpu
from jax.sharding import PartitionSpec as P


STEPS = 4
NS_ITERS = 4
REGION_VALUES = 256

step_size = 0.05
coupling = 0.4

VMEM = pl.BlockSpec(memory_space=pltpu.VMEM)
ANY = pl.BlockSpec(memory_space=pl.ANY)
SMEM = pl.BlockSpec(memory_space=pltpu.SMEM)
GRANT = 16 * 1024 * 1024


def params():
    return pltpu.CompilerParams(vmem_limit_bytes=GRANT)


def pack_kernel(strip_ref, ens_ref, forcing_ref, cross_ref, near_ref):
    odd = lax.rem(strip_ref[0], 2)
    for parity, low, high in ((0, cross_ref, near_ref), (1, near_ref, cross_ref)):

        @pl.when(odd == parity)
        def _():
            for row in range(STEPS):
                low[row] = ens_ref[:, row, :]
                high[row] = ens_ref[:, STEPS + row, :]

    cross_ref[STEPS] = forcing_ref[...]
    near_ref[STEPS] = forcing_ref[...]


def columns_kernel(count_ref, index_ref, value_ref, precision_ref, after_ref, columns_ref):
    slots = index_ref.shape[1]
    slot = lax.broadcasted_iota(jnp.int32, (1, slots), 1)
    lines = []
    for region in range(index_ref.shape[0]):
        live = (slot < count_ref[region]).astype(jnp.float32)
        weight = precision_ref[region : region + 1, :] * live
        lines += [
            index_ref[region : region + 1, :].astype(jnp.float32),
            jnp.sqrt(weight),
            value_ref[region : region + 1, :],
            weight,
        ]
    columns_ref[...] = jnp.concatenate(lines, axis=0).T


def forecast_kernel(last, strip_ref, after_ref, own_near_ref, own_cross_ref, got_near_ref, got_cross_ref, out_ref, even_ref, other_ref, forcing_ref):
    strip = strip_ref[0]
    odd = lax.rem(strip, 2)
    rows = 2 * STEPS
    lon = out_ref.shape[0] * out_ref.shape[2] // rows
    own_cross_at = STEPS + STEPS * odd
    own_near_at = 2 * STEPS - STEPS * odd
    got_cross_at = 3 * STEPS * odd
    got_near_at = 3 * STEPS - 3 * STEPS * odd
    for row in range(STEPS):
        even_ref[own_cross_at + row] = own_cross_ref[row]
        even_ref[own_near_at + row] = own_near_ref[row]
        even_ref[got_cross_at + row] = got_cross_ref[row]
        even_ref[got_near_at + row] = got_near_ref[row]
    forcing_ref[1] = own_near_ref[STEPS]
    forcing_ref[2 * odd] = got_cross_ref[STEPS]
    forcing_ref[2 - 2 * odd] = got_near_ref[STEPS]
    buffers = (even_ref, other_ref)
    for step in range(STEPS):
        source, target = buffers[step % 2], buffers[(step + 1) % 2]
        final = step == STEPS - 1

        def advance(row, carry):
            center = source[row]
            around = source[row - 1] + source[row + 1]
            far = row + rows - STEPS
            force = forcing_ref[far // rows, pl.ds(lax.rem(far, rows), 1), :]
            west = pltpu.roll(center, 1, 1)
            west2 = pltpu.roll(center, 2, 1)
            east = pltpu.roll(center, lon - 1, 1)
            new = (
                center * (1.0 - step_size - 2.0 * coupling)
                + step_size * ((east - west2) * west + force)
                + coupling * around
            )
            if final:
                parts = lon // out_ref.shape[2]
                for part in range(parts):
                    out_ref[(row - STEPS) * parts + part] = new[:, part * out_ref.shape[2] : (part + 1) * out_ref.shape[2]]
            else:
                below = jnp.logical_and(row < STEPS, strip == 0)
                above = jnp.logical_and(row >= STEPS + rows, strip == last)
                outside = jnp.logical_or(below, above)
                target[row] = new * jnp.where(outside, 0.0, 1.0)
            return carry

        lax.fori_loop(step + 1, rows + 2 * STEPS - 1 - step, advance, 0)


def halves(x):
    high = x.astype(jnp.bfloat16)
    return high, (x - high.astype(jnp.float32)).astype(jnp.bfloat16)


NN = (((1,), (0,)), ((), ()))
NT = (((1,), (1,)), ((), ()))


def dot(a, b, dims):
    return lax.dot_general(a, b, dims, preferred_element_type=jnp.float32)


def product(a, b, dims=NN):
    (ah, al), (bh, bl) = a, b
    return dot(ah, bh, dims) + (dot(ah, bl, dims) + dot(al, bh, dims))


def analysis_kernel(columns_ref, block_ref, out_ref):
    chunks, per, _ = block_ref.shape
    members = chunks * per
    slots = columns_ref.shape[0]
    regions = block_ref.shape[2] // REGION_VALUES
    top = members - 1.0
    columns = columns_ref[...]
    for region in range(regions):
        cells = slice(region * REGION_VALUES, (region + 1) * REGION_VALUES)
        block = block_ref[:, :, cells].reshape(members, REGION_VALUES)
        index, root, value, _ = (columns[:, 4 * region + i : 4 * region + i + 1] for i in range(4))
        mean = jnp.sum(block, axis=0, keepdims=True) * (1.0 / members)
        spread = block - mean
        spread_parts = halves(spread)
        cell = lax.broadcasted_iota(jnp.int32, (slots, REGION_VALUES), 1).astype(jnp.float32)
        chosen = cell == index
        onehot = chosen.astype(jnp.bfloat16)
        observed = dot(onehot, spread_parts[0], NT) + dot(onehot, spread_parts[1], NT)
        obs_mean = jnp.sum(jnp.where(chosen, mean, 0.0), axis=1, keepdims=True)
        scaled = observed * root
        misfit = root * (value - obs_mean)
        scaled_parts = halves(scaled)
        small = product(scaled_parts, scaled_parts, NT)
        carried = product(scaled_parts, spread_parts)
        norm = top + jnp.sqrt(jnp.sum(small * small, keepdims=True))
        inverse = 1.0 / norm
        eye = (
            lax.broadcasted_iota(jnp.int32, (slots, slots), 0)
            == lax.broadcasted_iota(jnp.int32, (slots, slots), 1)
        ).astype(jnp.float32)
        left = (top * eye + small) * inverse
        left_zero = top * inverse
        left_rest = inverse * eye
        right = right_rest = None
        right_zero = jnp.ones_like(norm)
        for repeat in range(NS_ITERS):
            fix = 1.5 * eye - 0.5 * left
            fix_zero = 1.5 - 0.5 * left_zero
            fix_parts = halves(fix)
            if repeat == 0:
                right, right_rest = fix, -0.5 * left_rest
            else:
                new_rest = -0.5 * right_zero * left_rest
                if repeat == 1:
                    right_rest = (-0.5 * inverse) * fix + new_rest
                else:
                    right_rest = product(halves(right_rest), fix_parts) + new_rest
                right = product(halves(right), fix_parts)
            right_zero = right_zero * fix_zero
            if repeat < NS_ITERS - 1:
                square = product(fix_parts, fix_parts)
                mixed = square - (0.5 * left_zero) * (fix + fix_zero * eye)
                if repeat == 0:
                    left_rest = inverse * mixed
                else:
                    left_rest = product(halves(left_rest), halves(mixed))
                left = product(halves(left), halves(square))
                left_zero = left_zero * fix_zero * fix_zero
        along = jnp.sum(right * misfit, axis=0, keepdims=True)
        twice = jnp.sum(right * along, axis=1, keepdims=True)
        moved = jnp.sum(twice * carried, axis=0, keepdims=True) * inverse
        pushed = product(halves(right_rest), halves(carried))
        gain = math.sqrt(top) * lax.rsqrt(norm)
        turned = halves(scaled.T)
        update = product(turned, halves(pushed))
        result = (mean + moved) + gain * (right_zero * spread + update)
        out_ref[:, :, cells] = result.reshape(chunks, per, REGION_VALUES)


def unpack_kernel(block_ref, out_ref):
    rows = out_ref.shape[1]
    parts = block_ref.shape[0] // rows
    width = block_ref.shape[2]
    for row in range(rows):
        for part in range(parts):
            out_ref[:, row, part * width : (part + 1) * width] = block_ref[row * parts + part]


def local(ensemble, forcing, obs_index, obs_count, obs_value, obs_precision):
    per, rows, lon = ensemble.shape
    strips = lax.axis_size("strip")
    strip = lax.axis_index("strip").astype(jnp.int32).reshape(1)
    regions, slots = obs_index.shape
    slab = jax.ShapeDtypeStruct((STEPS + 1, per, lon), jnp.float32)

    cross, near = pl.pallas_call(
        pack_kernel,
        out_shape=(slab, slab),
        in_specs=[SMEM, VMEM, VMEM],
        out_specs=(VMEM, VMEM),
        compiler_params=params(),
        name="pack",
    )(strip, ensemble, forcing)
    span = [(i, i + 1) for i in range(1, strips - 1, 2)]
    span = span + [(b, a) for a, b in span]
    swap = [(i, i ^ 1) for i in range(strips)]
    got_cross = lax.ppermute(cross, "strip", span)
    got_near = lax.ppermute(near, "strip", swap)
    columns = pl.pallas_call(
        columns_kernel,
        out_shape=jax.ShapeDtypeStruct((slots, 4 * regions), jnp.float32),
        in_specs=[SMEM] + [VMEM] * 3 + [ANY],
        out_specs=VMEM,
        compiler_params=params(),
        cost_estimate=pl.CostEstimate(flops=10**7, bytes_accessed=4096, transcendentals=0),
        name="columns",
    )(obs_count, obs_index, obs_value, obs_precision, near)
    chunks = lax.axis_size("mem")
    width = rows * lon // chunks
    sent = pl.pallas_call(
        functools.partial(forecast_kernel, strips - 1),
        out_shape=jax.ShapeDtypeStruct((chunks, per, width), jnp.float32),
        in_specs=[SMEM, ANY] + [VMEM] * 4,
        out_specs=VMEM,
        scratch_shapes=[
            pltpu.VMEM((4 * STEPS, per, lon), jnp.float32),
            pltpu.VMEM((4 * STEPS, per, lon), jnp.float32),
            pltpu.VMEM((3, rows, lon), jnp.float32),
        ],
        compiler_params=params(),
        name="forecast",
    )(strip, columns, near, cross, got_near, got_cross)
    regional = lax.all_to_all(sent, "mem", split_axis=0, concat_axis=0, tiled=True)
    analysed = pl.pallas_call(
        analysis_kernel,
        out_shape=jax.ShapeDtypeStruct((chunks, per, width), jnp.float32),
        in_specs=[VMEM] * 2,
        out_specs=VMEM,
        compiler_params=params(),
        name="analysis",
    )(columns, regional)
    back = lax.all_to_all(analysed, "mem", split_axis=0, concat_axis=0, tiled=True)
    return pl.pallas_call(
        unpack_kernel,
        out_shape=jax.ShapeDtypeStruct((per, rows, lon), jnp.float32),
        in_specs=[VMEM],
        out_specs=VMEM,
        compiler_params=params(),
        name="unpack",
    )(back)


def solution(mesh):
    placed = (
        P("mem", "strip", None),
        P("strip", None),
        P(("strip", "mem"), None),
        P(("strip", "mem")),
        P(("strip", "mem"), None),
        P(("strip", "mem"), None),
    )
    return jax.shard_map(
        local, mesh=mesh, in_specs=placed, out_specs=P("mem", "strip", None), check_vma=False
    )
```

```python
import functools
import math

import jax
import jax.numpy as jnp
from jax import lax
from jax.experimental import pallas as pl
from jax.experimental.pallas import tpu as pltpu
from jax.sharding import PartitionSpec as P


STEPS = 4
NS_ITERS = 4
REGION_VALUES = 256

step_size = 0.05
coupling = 0.4

VMEM = pl.BlockSpec(memory_space=pltpu.VMEM)
ANY = pl.BlockSpec(memory_space=pl.ANY)
SMEM = pl.BlockSpec(memory_space=pltpu.SMEM)
GRANT = 16 * 1024 * 1024


def params():
    return pltpu.CompilerParams(vmem_limit_bytes=GRANT)


def pack_kernel(strip_ref, ens_ref, forcing_ref, cross_ref, near_ref):
    odd = lax.rem(strip_ref[0], 2)
    for parity, low, high in ((0, cross_ref, near_ref), (1, near_ref, cross_ref)):

        @pl.when(odd == parity)
        def _():
            for row in range(STEPS):
                low[row] = ens_ref[:, row, :]
                high[row] = ens_ref[:, STEPS + row, :]

    cross_ref[STEPS] = forcing_ref[...]
    near_ref[STEPS] = forcing_ref[...]


def columns_kernel(count_ref, index_ref, value_ref, precision_ref, after_ref, columns_ref):
    slots = index_ref.shape[1]
    slot = lax.broadcasted_iota(jnp.int32, (1, slots), 1)
    lines = []
    for region in range(index_ref.shape[0]):
        live = (slot < count_ref[region]).astype(jnp.float32)
        weight = precision_ref[region : region + 1, :] * live
        lines += [
            index_ref[region : region + 1, :].astype(jnp.float32),
            jnp.sqrt(weight),
            value_ref[region : region + 1, :],
            weight,
        ]
    columns_ref[...] = jnp.concatenate(lines, axis=0).T


def forecast_kernel(last, strip_ref, after_ref, own_near_ref, own_cross_ref, got_near_ref, got_cross_ref, out_ref, even_ref, other_ref, forcing_ref):
    strip = strip_ref[0]
    odd = lax.rem(strip, 2)
    rows = 2 * STEPS
    lon = out_ref.shape[0] * out_ref.shape[2] // rows
    own_cross_at = STEPS + STEPS * odd
    own_near_at = 2 * STEPS - STEPS * odd
    got_cross_at = 3 * STEPS * odd
    got_near_at = 3 * STEPS - 3 * STEPS * odd
    for row in range(STEPS):
        even_ref[own_cross_at + row] = own_cross_ref[row]
        even_ref[own_near_at + row] = own_near_ref[row]
        even_ref[got_cross_at + row] = got_cross_ref[row]
        even_ref[got_near_at + row] = got_near_ref[row]
    forcing_ref[1] = own_near_ref[STEPS]
    forcing_ref[2 * odd] = got_cross_ref[STEPS]
    forcing_ref[2 - 2 * odd] = got_near_ref[STEPS]
    low_kept = jnp.where(strip == 0, 0.0, 1.0)
    high_kept = jnp.where(strip == last, 0.0, 1.0)
    buffers = (even_ref, other_ref)
    for step in range(STEPS):
        source, target = buffers[step % 2], buffers[(step + 1) % 2]
        final = step == STEPS - 1

        for row in range(step + 1, rows + 2 * STEPS - 1 - step):
            center = source[row]
            around = source[row - 1] + source[row + 1]
            far = row + rows - STEPS
            force = forcing_ref[far // rows, far % rows : far % rows + 1, :]
            west = pltpu.roll(center, 1, 1)
            west2 = pltpu.roll(center, 2, 1)
            east = pltpu.roll(center, lon - 1, 1)
            new = (
                center * (1.0 - step_size - 2.0 * coupling)
                + step_size * ((east - west2) * west + force)
                + coupling * around
            )
            if final:
                width = out_ref.shape[2]
                parts = lon // width
                for part in range(parts):
                    out_ref[(row - STEPS) * parts + part] = new[:, part * width : (part + 1) * width]
            elif row < STEPS:
                target[row] = new * low_kept
            elif row >= STEPS + rows:
                target[row] = new * high_kept
            else:
                target[row] = new


NN = (((1,), (0,)), ((), ()))
NT = (((1,), (1,)), ((), ()))


def halves(x):
    high = x.astype(jnp.bfloat16)
    return high, (x - high.astype(jnp.float32)).astype(jnp.bfloat16)


def dot(a, b, dims=NN):
    return lax.dot_general(a, b, dims, preferred_element_type=jnp.float32)


def across(parts):
    high, low = parts
    return jnp.concatenate([high, low, high], axis=1)


def down(parts):
    high, low = parts
    return jnp.concatenate([high, high, low], axis=0)


def stack(*parts):
    return tuple(jnp.concatenate(p, axis=0) for p in zip(*parts))


def product(a, b):
    return dot(across(a), down(b))


def analysis_kernel(columns_ref, block_ref, out_ref):
    chunks, per, _ = block_ref.shape
    members = chunks * per
    slots = columns_ref.shape[0]
    regions = block_ref.shape[2] // REGION_VALUES
    top = members - 1.0
    columns = columns_ref[...]
    eye = (lax.broadcasted_iota(jnp.int32, (slots, slots), 0) == lax.broadcasted_iota(jnp.int32, (slots, slots), 1)).astype(jnp.float32)
    cell = lax.broadcasted_iota(jnp.int32, (slots, REGION_VALUES), 1).astype(jnp.float32)

    def begin(r):
        cells = slice(r * REGION_VALUES, (r + 1) * REGION_VALUES)
        block = block_ref[:, :, cells].reshape(members, REGION_VALUES)
        index, root, value = (columns[:, 4 * r + i : 4 * r + i + 1] for i in range(3))
        mean = jnp.sum(block, axis=0, keepdims=True) * (1.0 / members)
        spread = block - mean
        sh, sl = halves(spread)
        chosen = cell == index
        onehot = chosen.astype(jnp.bfloat16)
        observed = dot(onehot, sh, NT) + dot(onehot, sl, NT)
        obs_mean = jnp.sum(jnp.where(chosen, mean, 0.0), axis=1, keepdims=True)
        scaled = observed * root
        misfit = root * (value - obs_mean)
        gh, gl = halves(scaled)
        small = dot(jnp.concatenate([gh, gl, gh], axis=1), jnp.concatenate([gh, gh, gl], axis=1), NT)
        carried = product((gh, gl), (sh, sl))
        norm = top + jnp.sqrt(jnp.sum(small * small, keepdims=True))
        inverse = 1.0 / norm
        return dict(mean=mean, scaled=scaled, misfit=misfit, carried=carried, norm=norm, inverse=inverse, small=small)

    def iterate(s):
        inverse = s["inverse"]
        left = (top * inverse) * eye + s["small"] * inverse
        left_zero = top * inverse
        fix = 1.5 * eye - 0.5 * left
        fix_zero = 1.5 - 0.5 * left_zero
        f = halves(fix)
        square = product(f, f)
        yield 2
        mixed = square - (0.5 * left_zero) * (fix + fix_zero * eye)
        left_rest = inverse * mixed
        left = product(halves(left), halves(square))
        yield 2
        right, right_zero, rest = fix, fix_zero, (-0.5 * inverse) * eye
        left_zero = left_zero * fix_zero * fix_zero
        for repeat in range(1, NS_ITERS):
            fix = 1.5 * eye - 0.5 * left
            fix_zero = 1.5 - 0.5 * left_zero
            f = halves(fix)
            last = repeat == NS_ITERS - 1
            rows = [halves(right)] if last else [f, halves(right), halves(left_rest)]
            if repeat > 1: rows.append(halves(rest))
            got = product(stack(*rows), f)
            got = [got[i * slots : (i + 1) * slots] for i in range(len(rows))]
            yield 2
            new_rest = (got[-1] if repeat > 1 else (-0.5 * inverse) * fix) - (0.5 * right_zero) * left_rest
            if not last:
                square, right, rest_fix = got[:3]
                both = product(stack(halves(left), halves(left_rest)), halves(square))
                left = both[:slots]
                left_rest = both[slots:] - (0.5 * left_zero) * (rest_fix + fix_zero * left_rest)
                left_zero = left_zero * fix_zero * fix_zero
                yield 2
            else:
                right = got[0]
            rest = new_rest
            right_zero = right_zero * fix_zero
        s.update(right=right, right_zero=right_zero, rest=rest)

    def finish(r, s):
        cells = slice(r * REGION_VALUES, (r + 1) * REGION_VALUES)
        right, carried = s["right"], s["carried"]
        along = jnp.sum(right * s["misfit"], axis=0, keepdims=True)
        twice = jnp.sum(right * along, axis=1, keepdims=True)
        moved = jnp.sum(twice * carried, axis=0, keepdims=True) * s["inverse"]
        pushed = product(halves(s["rest"]), halves(carried))
        gain = math.sqrt(top) * lax.rsqrt(s["norm"])
        update = product(halves(s["scaled"].T * gain), halves(pushed))
        block = block_ref[:, :, cells].reshape(members, REGION_VALUES)
        keep = gain * s["right_zero"]
        result = keep * block + (s["mean"] * (1.0 - keep) + moved) + update
        out_ref[:, :, cells] = result.reshape(chunks, per, REGION_VALUES)

    states = [begin(r) for r in range(regions)]
    runs = [iterate(s) for s in states]
    while runs:
        runs = [run for run in runs if next(run, 0)]
    for r in range(regions):
        finish(r, states[r])


def unpack_kernel(block_ref, out_ref):
    rows = out_ref.shape[1]
    parts = block_ref.shape[0] // rows
    width = block_ref.shape[2]
    for row in range(rows):
        for part in range(parts):
            out_ref[:, row, part * width : (part + 1) * width] = block_ref[row * parts + part]


def local(ensemble, forcing, obs_index, obs_count, obs_value, obs_precision):
    per, rows, lon = ensemble.shape
    strips = lax.axis_size("strip")
    strip = lax.axis_index("strip").astype(jnp.int32).reshape(1)
    regions, slots = obs_index.shape
    slab = jax.ShapeDtypeStruct((STEPS + 1, per, lon), jnp.float32)

    cross, near = pl.pallas_call(
        pack_kernel,
        out_shape=(slab, slab),
        in_specs=[SMEM, VMEM, VMEM],
        out_specs=(VMEM, VMEM),
        compiler_params=params(),
        name="pack",
    )(strip, ensemble, forcing)
    span = [(i, i + 1) for i in range(1, strips - 1, 2)]
    span = span + [(b, a) for a, b in span]
    swap = [(i, i ^ 1) for i in range(strips)]
    got_cross = lax.ppermute(cross, "strip", span)
    got_near = lax.ppermute(near, "strip", swap)
    columns = pl.pallas_call(
        columns_kernel,
        out_shape=jax.ShapeDtypeStruct((slots, 4 * regions), jnp.float32),
        in_specs=[SMEM] + [VMEM] * 3 + [ANY],
        out_specs=VMEM,
        compiler_params=params(),
        cost_estimate=pl.CostEstimate(flops=10**7, bytes_accessed=4096, transcendentals=0),
        name="columns",
    )(obs_count, obs_index, obs_value, obs_precision, near)
    chunks = lax.axis_size("mem")
    width = rows * lon // chunks
    sent = pl.pallas_call(
        functools.partial(forecast_kernel, strips - 1),
        out_shape=jax.ShapeDtypeStruct((chunks, per, width), jnp.float32),
        in_specs=[SMEM, ANY] + [VMEM] * 4,
        out_specs=VMEM,
        scratch_shapes=[
            pltpu.VMEM((4 * STEPS, per, lon), jnp.float32),
            pltpu.VMEM((4 * STEPS, per, lon), jnp.float32),
            pltpu.VMEM((3, rows, lon), jnp.float32),
        ],
        compiler_params=params(),
        name="forecast",
    )(strip, columns, near, cross, got_near, got_cross)
    regional = lax.all_to_all(sent, "mem", split_axis=0, concat_axis=0, tiled=True)
    analysed = pl.pallas_call(
        analysis_kernel,
        out_shape=jax.ShapeDtypeStruct((chunks, per, width), jnp.float32),
        in_specs=[VMEM] * 2,
        out_specs=VMEM,
        compiler_params=params(),
        name="analysis",
    )(columns, regional)
    back = lax.all_to_all(analysed, "mem", split_axis=0, concat_axis=0, tiled=True)
    return pl.pallas_call(
        unpack_kernel,
        out_shape=jax.ShapeDtypeStruct((per, rows, lon), jnp.float32),
        in_specs=[VMEM],
        out_specs=VMEM,
        compiler_params=params(),
        name="unpack",
    )(back)


def solution(mesh):
    placed = (
        P("mem", "strip", None),
        P("strip", None),
        P(("strip", "mem"), None),
        P(("strip", "mem")),
        P(("strip", "mem"), None),
        P(("strip", "mem"), None),
    )
    return jax.shard_map(local, mesh=mesh, in_specs=placed, out_specs=P("mem", "strip", None), check_vma=False)
```

```python
import functools
import math

import jax
import jax.numpy as jnp
from jax import lax
from jax.experimental import pallas as pl
from jax.experimental.pallas import tpu as pltpu
from jax.sharding import PartitionSpec as P


STEPS = 4
NS_ITERS = 4
REGION_VALUES = 256

step_size = 0.05
coupling = 0.4

VMEM = pl.BlockSpec(memory_space=pltpu.VMEM)
ANY = pl.BlockSpec(memory_space=pl.ANY)
SMEM = pl.BlockSpec(memory_space=pltpu.SMEM)
GRANT = 16 * 1024 * 1024


def params():
    return pltpu.CompilerParams(vmem_limit_bytes=GRANT)


def row_of(line, parity):
    return line if parity == 0 else 2 * STEPS - 1 - line


def pack_kernel(strip_ref, ens_ref, forcing_ref, cross_ref, near_ref):
    odd = lax.rem(strip_ref[0], 2)
    half = cross_ref.shape[2]
    for parity in (0, 1):

        @pl.when(odd == parity)
        def _():
            for line in range(2 * STEPS):
                message = cross_ref if line < STEPS else near_ref
                at, row = line % STEPS, row_of(line, parity)
                state, force = ens_ref[:, row, :], forcing_ref[row : row + 1, :]
                for side in range(2):
                    lons = slice(side * half, (side + 1) * half)
                    message[2 * at + side] = state[:, lons]
                    spot = side * STEPS + at
                    message[2 * STEPS, spot : spot + 1, :] = force[:, lons]


def columns_kernel(count_ref, index_ref, value_ref, precision_ref, after_ref, columns_ref):
    slots = index_ref.shape[1]
    slot = lax.broadcasted_iota(jnp.int32, (1, slots), 1)
    lines = []
    for region in range(index_ref.shape[0]):
        live = (slot < count_ref[region]).astype(jnp.float32)
        weight = precision_ref[region : region + 1, :] * live
        lines += [
            index_ref[region : region + 1, :].astype(jnp.float32),
            jnp.sqrt(weight),
            value_ref[region : region + 1, :],
            weight,
        ]
    columns_ref[...] = jnp.concatenate(lines, axis=0).T


def state_of(message, at):
    return jnp.concatenate([message[2 * at], message[2 * at + 1]], axis=1)


def force_of(message, at):
    both = [message[2 * STEPS, spot : spot + 1, :] for spot in (at, STEPS + at)]
    return jnp.concatenate(both, axis=1)


def advance(before, center, after, force):
    lon = center.shape[1]
    west = pltpu.roll(center, 1, 1)
    west2 = pltpu.roll(center, 2, 1)
    east = pltpu.roll(center, lon - 1, 1)
    return (
        center * (1.0 - step_size - 2.0 * coupling)
        + step_size * ((east - west2) * west + force)
        + coupling * (before + after)
    )


def put_line(out_ref, odd, line, value):
    width = out_ref.shape[2]
    parts = value.shape[1] // width
    for parity in (0, 1):

        @pl.when(odd == parity)
        def _():
            for part in range(parts):
                chunk = row_of(line, parity) * parts + part
                out_ref[chunk] = value[:, part * width : (part + 1) * width]


def near_kernel(after_ref, own_cross_ref, own_near_ref, got_near_ref, done_ref, edge_ref, *levels):
    def start(read):
        def of(line):
            if line < STEPS:
                return read(own_cross_ref, line)
            if line < 2 * STEPS:
                return read(own_near_ref, line - STEPS)
            return read(got_near_ref, 3 * STEPS - 1 - line)

        return of

    force = start(force_of)
    read = start(state_of)
    for step in range(1, STEPS + 1):
        for line in range(step, 3 * STEPS - step):
            new = advance(read(line - 1), read(line), read(line + 1), force(line))
            if step == STEPS:
                done_ref[line - STEPS] = new
            else:
                levels[step - 1][line - step] = new
                if line < step + 2:
                    edge_ref[2 * (step - 1) + line - step] = new
        if step < STEPS:
            read = lambda line, step=step: levels[step - 1][line - step]


def cross_kernel(last, strip_ref, done_ref, own_cross_ref, got_cross_ref, edge_ref, out_ref, *levels):
    strip = strip_ref[0]
    odd = lax.rem(strip, 2)
    kept = jnp.where(jnp.logical_or(strip == 0, strip == last), 0.0, 1.0)

    def start(read):
        return lambda line: read(own_cross_ref, line) if line >= 0 else read(got_cross_ref, -1 - line)

    for line in range(STEPS):
        put_line(out_ref, odd, STEPS + line, done_ref[line])
    force = start(force_of)
    read = start(state_of)
    for step in range(1, STEPS + 1):
        first = step - STEPS
        for line in range(first, first + STEPS):
            new = advance(read(line - 1), read(line), read(line + 1), force(line))
            if line < 0:
                new = new * kept
            if step == STEPS:
                put_line(out_ref, odd, line, new)
            else:
                levels[step - 1][line - first] = new
        if step < STEPS:

            def read(line, step=step, first=first):
                if line < step:
                    return levels[step - 1][line - first]
                return edge_ref[2 * (step - 1) + line - step]


NN = (((1,), (0,)), ((), ()))
NT = (((1,), (1,)), ((), ()))


def halves(x):
    high = x.astype(jnp.bfloat16)
    return high, (x - high.astype(jnp.float32)).astype(jnp.bfloat16)


def dot(a, b, dims=NN):
    return lax.dot_general(a, b, dims, preferred_element_type=jnp.float32)


def across(parts):
    high, low = parts
    return jnp.concatenate([high, low, high], axis=1)


def down(parts):
    high, low = parts
    return jnp.concatenate([high, high, low], axis=0)


def stack(*parts):
    return tuple(jnp.concatenate(p, axis=0) for p in zip(*parts))


def product(a, b):
    return dot(across(a), down(b))


def analysis_kernel(columns_ref, block_ref, out_ref):
    chunks, per, _ = block_ref.shape
    members = chunks * per
    slots = columns_ref.shape[0]
    regions = block_ref.shape[2] // REGION_VALUES
    top = members - 1.0
    columns = columns_ref[...]
    eye = (lax.broadcasted_iota(jnp.int32, (slots, slots), 0) == lax.broadcasted_iota(jnp.int32, (slots, slots), 1)).astype(jnp.float32)
    cell = lax.broadcasted_iota(jnp.int32, (slots, REGION_VALUES), 1).astype(jnp.float32)

    def begin(r):
        cells = slice(r * REGION_VALUES, (r + 1) * REGION_VALUES)
        block = block_ref[:, :, cells].reshape(members, REGION_VALUES)
        index, root, value = (columns[:, 4 * r + i : 4 * r + i + 1] for i in range(3))
        mean = jnp.sum(block, axis=0, keepdims=True) * (1.0 / members)
        spread = block - mean
        sh, sl = halves(spread)
        chosen = cell == index
        onehot = chosen.astype(jnp.bfloat16)
        observed = dot(onehot, sh, NT) + dot(onehot, sl, NT)
        obs_mean = jnp.sum(jnp.where(chosen, mean, 0.0), axis=1, keepdims=True)
        scaled = observed * root
        misfit = root * (value - obs_mean)
        gh, gl = halves(scaled)
        small = dot(jnp.concatenate([gh, gl, gh], axis=1), jnp.concatenate([gh, gh, gl], axis=1), NT)
        carried = product((gh, gl), (sh, sl))
        norm = top + jnp.sqrt(jnp.sum(small * small, keepdims=True))
        inverse = 1.0 / norm
        return dict(mean=mean, scaled=scaled, misfit=misfit, carried=carried, norm=norm, inverse=inverse, small=small)

    def iterate(s):
        inverse = s["inverse"]
        left = (top * inverse) * eye + s["small"] * inverse
        left_zero = top * inverse
        fix = 1.5 * eye - 0.5 * left
        fix_zero = 1.5 - 0.5 * left_zero
        f = halves(fix)
        square = product(f, f)
        yield 2
        mixed = square - (0.5 * left_zero) * (fix + fix_zero * eye)
        left_rest = inverse * mixed
        left = product(halves(left), halves(square))
        yield 2
        right, right_zero, rest = fix, fix_zero, (-0.5 * inverse) * eye
        left_zero = left_zero * fix_zero * fix_zero
        for repeat in range(1, NS_ITERS):
            fix = 1.5 * eye - 0.5 * left
            fix_zero = 1.5 - 0.5 * left_zero
            f = halves(fix)
            last = repeat == NS_ITERS - 1
            rows = [halves(right)] if last else [f, halves(right), halves(left_rest)]
            if repeat > 1: rows.append(halves(rest))
            got = product(stack(*rows), f)
            got = [got[i * slots : (i + 1) * slots] for i in range(len(rows))]
            yield 2
            new_rest = (got[-1] if repeat > 1 else (-0.5 * inverse) * fix) - (0.5 * right_zero) * left_rest
            if not last:
                square, right, rest_fix = got[:3]
                both = product(stack(halves(left), halves(left_rest)), halves(square))
                left = both[:slots]
                left_rest = both[slots:] - (0.5 * left_zero) * (rest_fix + fix_zero * left_rest)
                left_zero = left_zero * fix_zero * fix_zero
                yield 2
            else:
                right = got[0]
            rest = new_rest
            right_zero = right_zero * fix_zero
        s.update(right=right, right_zero=right_zero, rest=rest)

    def finish(r, s):
        cells = slice(r * REGION_VALUES, (r + 1) * REGION_VALUES)
        right, carried = s["right"], s["carried"]
        along = jnp.sum(right * s["misfit"], axis=0, keepdims=True)
        twice = jnp.sum(right * along, axis=1, keepdims=True)
        moved = jnp.sum(twice * carried, axis=0, keepdims=True) * s["inverse"]
        pushed = product(halves(s["rest"]), halves(carried))
        gain = math.sqrt(top) * lax.rsqrt(s["norm"])
        update = product(halves(s["scaled"].T * gain), halves(pushed))
        block = block_ref[:, :, cells].reshape(members, REGION_VALUES)
        keep = gain * s["right_zero"]
        result = keep * block + (s["mean"] * (1.0 - keep) + moved) + update
        out_ref[:, :, cells] = result.reshape(chunks, per, REGION_VALUES)

    states = [begin(r) for r in range(regions)]
    runs = [iterate(s) for s in states]
    while runs:
        runs = [run for run in runs if next(run, 0)]
    for r in range(regions):
        finish(r, states[r])


def unpack_kernel(block_ref, out_ref):
    rows = out_ref.shape[1]
    parts = block_ref.shape[0] // rows
    width = block_ref.shape[2]
    for row in range(rows):
        for part in range(parts):
            out_ref[:, row, part * width : (part + 1) * width] = block_ref[row * parts + part]


def local(ensemble, forcing, obs_index, obs_count, obs_value, obs_precision):
    per, rows, lon = ensemble.shape
    strips = lax.axis_size("strip")
    strip = lax.axis_index("strip").astype(jnp.int32).reshape(1)
    regions, slots = obs_index.shape
    message = jax.ShapeDtypeStruct((2 * STEPS + 1, per, lon // 2), jnp.float32)

    cross, near = pl.pallas_call(
        pack_kernel,
        out_shape=(message, message),
        in_specs=[SMEM, VMEM, VMEM],
        out_specs=(VMEM, VMEM),
        compiler_params=params(),
        name="pack",
    )(strip, ensemble, forcing)
    span = [(i, i + 1) for i in range(1, strips - 1, 2)]
    span = span + [(b, a) for a, b in span]
    swap = [(i, i ^ 1) for i in range(strips)]
    got_cross = lax.ppermute(cross, "strip", span)
    got_near = lax.ppermute(near, "strip", swap)
    columns = pl.pallas_call(
        columns_kernel,
        out_shape=jax.ShapeDtypeStruct((slots, 4 * regions), jnp.float32),
        in_specs=[SMEM] + [VMEM] * 3 + [ANY],
        out_specs=VMEM,
        compiler_params=params(),
        cost_estimate=pl.CostEstimate(flops=10**7, bytes_accessed=4096, transcendentals=0),
        name="columns",
    )(obs_count, obs_index, obs_value, obs_precision, near)
    chunks = lax.axis_size("mem")
    width = rows * lon // chunks
    full = jax.ShapeDtypeStruct((chunks, per, width), jnp.float32)

    def line_slabs(count):
        return pltpu.VMEM((count, per, lon), jnp.float32)

    done, edges = pl.pallas_call(
        near_kernel,
        out_shape=tuple(jax.ShapeDtypeStruct((count, per, lon), jnp.float32) for count in (STEPS, 2 * (STEPS - 1))),
        in_specs=[ANY] + [VMEM] * 3,
        out_specs=(VMEM, VMEM),
        scratch_shapes=[line_slabs(3 * STEPS - 2 * step) for step in range(1, STEPS)],
        compiler_params=params(),
        cost_estimate=pl.CostEstimate(flops=10**8, bytes_accessed=4096, transcendentals=0),
        name="forecast_near",
    )(columns, cross, near, got_near)
    sent = pl.pallas_call(
        functools.partial(cross_kernel, strips - 1),
        out_shape=full,
        in_specs=[SMEM] + [VMEM] * 4,
        out_specs=VMEM,
        scratch_shapes=[line_slabs(STEPS) for _ in range(1, STEPS)],
        compiler_params=params(),
        name="forecast_cross",
    )(strip, done, cross, got_cross, edges)
    regional = lax.all_to_all(sent, "mem", split_axis=0, concat_axis=0, tiled=True)
    analysed = pl.pallas_call(
        analysis_kernel,
        out_shape=jax.ShapeDtypeStruct((chunks, per, width), jnp.float32),
        in_specs=[VMEM] * 2,
        out_specs=VMEM,
        compiler_params=params(),
        name="analysis",
    )(columns, regional)
    back = lax.all_to_all(analysed, "mem", split_axis=0, concat_axis=0, tiled=True)
    return pl.pallas_call(
        unpack_kernel,
        out_shape=jax.ShapeDtypeStruct((per, rows, lon), jnp.float32),
        in_specs=[VMEM],
        out_specs=VMEM,
        compiler_params=params(),
        name="unpack",
    )(back)


def solution(mesh):
    placed = (
        P("mem", "strip", None),
        P("strip", None),
        P(("strip", "mem"), None),
        P(("strip", "mem")),
        P(("strip", "mem"), None),
        P(("strip", "mem"), None),
    )
    return jax.shard_map(local, mesh=mesh, in_specs=placed, out_specs=P("mem", "strip", None), check_vma=False)
```

```python
import functools
import math

import jax
import jax.numpy as jnp
from jax import lax
from jax.experimental import pallas as pl
from jax.experimental.pallas import tpu as pltpu
from jax.sharding import PartitionSpec as P


STEPS = 4
NS_ITERS = 4
REGION_VALUES = 256

step_size = 0.05
coupling = 0.4

VMEM = pl.BlockSpec(memory_space=pltpu.VMEM)
ANY = pl.BlockSpec(memory_space=pl.ANY)
SMEM = pl.BlockSpec(memory_space=pltpu.SMEM)
GRANT = 16 * 1024 * 1024


def params():
    return pltpu.CompilerParams(vmem_limit_bytes=GRANT)


LEAD = 20


def rank_of(owner, count):
    return (owner - LEAD) % count


def row_of(line, parity):
    return line if parity == 0 else 2 * STEPS - 1 - line


def pack_kernel(strip_ref, ens_ref, forcing_ref, cross_ref, near_ref):
    odd = lax.rem(strip_ref[0], 2)
    half = cross_ref.shape[2]
    for parity in (0, 1):

        @pl.when(odd == parity)
        def _():
            for line in range(2 * STEPS):
                message = cross_ref if line < STEPS else near_ref
                at, row = line % STEPS, row_of(line, parity)
                state, force = ens_ref[:, row, :], forcing_ref[row : row + 1, :]
                for side in range(2):
                    lons = slice(side * half, (side + 1) * half)
                    message[2 * at + side] = state[:, lons]
                    spot = side * STEPS + at
                    message[2 * STEPS, spot : spot + 1, :] = force[:, lons]


def columns_kernel(count_ref, index_ref, value_ref, precision_ref, after_ref, columns_ref):
    slots = index_ref.shape[1]
    slot = lax.broadcasted_iota(jnp.int32, (1, slots), 1)
    lines = []
    for region in range(index_ref.shape[0]):
        live = (slot < count_ref[region]).astype(jnp.float32)
        weight = precision_ref[region : region + 1, :] * live
        lines += [
            index_ref[region : region + 1, :].astype(jnp.float32),
            jnp.sqrt(weight),
            value_ref[region : region + 1, :],
            weight,
        ]
    columns_ref[...] = jnp.concatenate(lines, axis=0).T


def state_of(message, at):
    return jnp.concatenate([message[2 * at], message[2 * at + 1]], axis=1)


def force_of(message, at):
    both = [message[2 * STEPS, spot : spot + 1, :] for spot in (at, STEPS + at)]
    return jnp.concatenate(both, axis=1)


def advance(before, center, after, force):
    lon = center.shape[1]
    west = pltpu.roll(center, 1, 1)
    west2 = pltpu.roll(center, 2, 1)
    east = pltpu.roll(center, lon - 1, 1)
    return (
        center * (1.0 - step_size - 2.0 * coupling)
        + step_size * ((east - west2) * west + force)
        + coupling * (before + after)
    )


def put_line(out_ref, odd, line, value):
    width = out_ref.shape[2]
    parts = value.shape[1] // width
    for parity in (0, 1):

        @pl.when(odd == parity)
        def _():
            for part in range(parts):
                chunk = rank_of(row_of(line, parity) * parts + part, out_ref.shape[0])
                out_ref[chunk] = value[:, part * width : (part + 1) * width]


def near_kernel(after_ref, own_cross_ref, own_near_ref, got_near_ref, done_ref, edge_ref, *levels):
    def start(read):
        def of(line):
            if line < STEPS:
                return read(own_cross_ref, line)
            if line < 2 * STEPS:
                return read(own_near_ref, line - STEPS)
            return read(got_near_ref, 3 * STEPS - 1 - line)

        return of

    force = start(force_of)
    read = start(state_of)
    for step in range(1, STEPS + 1):
        for line in range(step, 3 * STEPS - step):
            new = advance(read(line - 1), read(line), read(line + 1), force(line))
            if step == STEPS:
                done_ref[line - STEPS] = new
            else:
                levels[step - 1][line - step] = new
                if line < step + 2:
                    edge_ref[2 * (step - 1) + line - step] = new
        if step < STEPS:
            read = lambda line, step=step: levels[step - 1][line - step]


def cross_kernel(last, strip_ref, done_ref, own_cross_ref, got_cross_ref, edge_ref, out_ref, *levels):
    strip = strip_ref[0]
    odd = lax.rem(strip, 2)
    kept = jnp.where(jnp.logical_or(strip == 0, strip == last), 0.0, 1.0)

    def start(read):
        return lambda line: read(own_cross_ref, line) if line >= 0 else read(got_cross_ref, -1 - line)

    for line in range(STEPS):
        put_line(out_ref, odd, STEPS + line, done_ref[line])
    force = start(force_of)
    read = start(state_of)
    for step in range(1, STEPS + 1):
        first = step - STEPS
        for line in range(first, first + STEPS):
            new = advance(read(line - 1), read(line), read(line + 1), force(line))
            if line < 0:
                new = new * kept
            if step == STEPS:
                put_line(out_ref, odd, line, new)
            else:
                levels[step - 1][line - first] = new
        if step < STEPS:

            def read(line, step=step, first=first):
                if line < step:
                    return levels[step - 1][line - first]
                return edge_ref[2 * (step - 1) + line - step]


NN = (((1,), (0,)), ((), ()))
NT = (((1,), (1,)), ((), ()))


def halves(x):
    high = x.astype(jnp.bfloat16)
    return high, (x - high.astype(jnp.float32)).astype(jnp.bfloat16)


def dot(a, b, dims=NN):
    return lax.dot_general(a, b, dims, preferred_element_type=jnp.float32)


def across(parts):
    high, low = parts
    return jnp.concatenate([high, low, high], axis=1)


def down(parts):
    high, low = parts
    return jnp.concatenate([high, high, low], axis=0)


def stack(*parts):
    return tuple(jnp.concatenate(p, axis=0) for p in zip(*parts))


def product(a, b):
    return dot(across(a), down(b))


def analysis_kernel(columns_ref, block_ref, out_ref):
    chunks, per, _ = block_ref.shape
    members = chunks * per
    slots = columns_ref.shape[0]
    regions = block_ref.shape[2] // REGION_VALUES
    top = members - 1.0
    columns = columns_ref[...]
    eye = (lax.broadcasted_iota(jnp.int32, (slots, slots), 0) == lax.broadcasted_iota(jnp.int32, (slots, slots), 1)).astype(jnp.float32)
    cell = lax.broadcasted_iota(jnp.int32, (slots, REGION_VALUES), 1).astype(jnp.float32)

    def begin(r):
        cells = slice(r * REGION_VALUES, (r + 1) * REGION_VALUES)
        block = block_ref[:, :, cells].reshape(members, REGION_VALUES)
        index, root, value = (columns[:, 4 * r + i : 4 * r + i + 1] for i in range(3))
        mean = jnp.sum(block, axis=0, keepdims=True) * (1.0 / members)
        spread = block - mean
        sh, sl = halves(spread)
        chosen = cell == index
        onehot = chosen.astype(jnp.bfloat16)
        observed = dot(onehot, sh, NT) + dot(onehot, sl, NT)
        obs_mean = jnp.sum(jnp.where(chosen, mean, 0.0), axis=1, keepdims=True)
        scaled = observed * root
        misfit = root * (value - obs_mean)
        gh, gl = halves(scaled)
        small = dot(jnp.concatenate([gh, gl, gh], axis=1), jnp.concatenate([gh, gh, gl], axis=1), NT)
        carried = product((gh, gl), (sh, sl))
        norm = top + jnp.sqrt(jnp.sum(small * small, keepdims=True))
        inverse = 1.0 / norm
        return dict(mean=mean, scaled=scaled, misfit=misfit, carried=carried, norm=norm, inverse=inverse, small=small)

    def iterate(s):
        inverse = s["inverse"]
        left = (top * inverse) * eye + s["small"] * inverse
        left_zero = top * inverse
        fix = 1.5 * eye - 0.5 * left
        fix_zero = 1.5 - 0.5 * left_zero
        f = halves(fix)
        square = product(f, f)
        yield 2
        mixed = square - (0.5 * left_zero) * (fix + fix_zero * eye)
        left_rest = inverse * mixed
        left = product(halves(left), halves(square))
        yield 2
        right, right_zero, rest = fix, fix_zero, (-0.5 * inverse) * eye
        left_zero = left_zero * fix_zero * fix_zero
        for repeat in range(1, NS_ITERS):
            fix = 1.5 * eye - 0.5 * left
            fix_zero = 1.5 - 0.5 * left_zero
            f = halves(fix)
            last = repeat == NS_ITERS - 1
            rows = [halves(right)] if last else [f, halves(right), halves(left_rest)]
            if repeat > 1: rows.append(halves(rest))
            got = product(stack(*rows), f)
            got = [got[i * slots : (i + 1) * slots] for i in range(len(rows))]
            yield 2
            new_rest = (got[-1] if repeat > 1 else (-0.5 * inverse) * fix) - (0.5 * right_zero) * left_rest
            if not last:
                square, right, rest_fix = got[:3]
                both = product(stack(halves(left), halves(left_rest)), halves(square))
                left = both[:slots]
                left_rest = both[slots:] - (0.5 * left_zero) * (rest_fix + fix_zero * left_rest)
                left_zero = left_zero * fix_zero * fix_zero
                yield 2
            else:
                right = got[0]
            rest = new_rest
            right_zero = right_zero * fix_zero
        s.update(right=right, right_zero=right_zero, rest=rest)

    def finish(r, s):
        cells = slice(r * REGION_VALUES, (r + 1) * REGION_VALUES)
        right, carried = s["right"], s["carried"]
        along = jnp.sum(right * s["misfit"], axis=0, keepdims=True)
        twice = jnp.sum(right * along, axis=1, keepdims=True)
        moved = jnp.sum(twice * carried, axis=0, keepdims=True) * s["inverse"]
        pushed = product(halves(s["rest"]), halves(carried))
        gain = math.sqrt(top) * lax.rsqrt(s["norm"])
        update = product(halves(s["scaled"].T * gain), halves(pushed))
        block = block_ref[:, :, cells].reshape(members, REGION_VALUES)
        keep = gain * s["right_zero"]
        result = keep * block + (s["mean"] * (1.0 - keep) + moved) + update
        out_ref[:, :, cells] = result.reshape(chunks, per, REGION_VALUES)

    states = [begin(r) for r in range(regions)]
    runs = [iterate(s) for s in states]
    while runs:
        runs = [run for run in runs if next(run, 0)]
    for r in range(regions):
        finish(r, states[r])


def unpack_kernel(block_ref, out_ref):
    rows = out_ref.shape[1]
    parts = block_ref.shape[0] // rows
    width = block_ref.shape[2]
    for row in range(rows):
        for part in range(parts):
            out_ref[:, row, part * width : (part + 1) * width] = block_ref[rank_of(row * parts + part, block_ref.shape[0])]


def local(ensemble, forcing, obs_index, obs_count, obs_value, obs_precision):
    per, rows, lon = ensemble.shape
    strips = lax.axis_size("strip")
    strip = lax.axis_index("strip").astype(jnp.int32).reshape(1)
    regions, slots = obs_index.shape
    message = jax.ShapeDtypeStruct((2 * STEPS + 1, per, lon // 2), jnp.float32)

    cross, near = pl.pallas_call(
        pack_kernel,
        out_shape=(message, message),
        in_specs=[SMEM, VMEM, VMEM],
        out_specs=(VMEM, VMEM),
        compiler_params=params(),
        name="pack",
    )(strip, ensemble, forcing)
    span = [(i, i + 1) for i in range(1, strips - 1, 2)]
    span = span + [(b, a) for a, b in span]
    swap = [(i, i ^ 1) for i in range(strips)]
    got_cross = lax.ppermute(cross, "strip", span)
    got_near = lax.ppermute(near, "strip", swap)
    columns = pl.pallas_call(
        columns_kernel,
        out_shape=jax.ShapeDtypeStruct((slots, 4 * regions), jnp.float32),
        in_specs=[SMEM] + [VMEM] * 3 + [ANY],
        out_specs=VMEM,
        compiler_params=params(),
        cost_estimate=pl.CostEstimate(flops=10**7, bytes_accessed=4096, transcendentals=0),
        name="columns",
    )(obs_count, obs_index, obs_value, obs_precision, near)
    chunks = lax.axis_size("mem")
    width = rows * lon // chunks
    full = jax.ShapeDtypeStruct((chunks, per, width), jnp.float32)

    def line_slabs(count):
        return pltpu.VMEM((count, per, lon), jnp.float32)

    done, edges = pl.pallas_call(
        near_kernel,
        out_shape=tuple(jax.ShapeDtypeStruct((count, per, lon), jnp.float32) for count in (STEPS, 2 * (STEPS - 1))),
        in_specs=[ANY] + [VMEM] * 3,
        out_specs=(VMEM, VMEM),
        scratch_shapes=[line_slabs(3 * STEPS - 2 * step) for step in range(1, STEPS)],
        compiler_params=params(),
        cost_estimate=pl.CostEstimate(flops=10**8, bytes_accessed=4096, transcendentals=0),
        name="forecast_near",
    )(columns, cross, near, got_near)
    sent = pl.pallas_call(
        functools.partial(cross_kernel, strips - 1),
        out_shape=full,
        in_specs=[SMEM] + [VMEM] * 4,
        out_specs=VMEM,
        scratch_shapes=[line_slabs(STEPS) for _ in range(1, STEPS)],
        compiler_params=params(),
        name="forecast_cross",
    )(strip, done, cross, got_cross, edges)
    ranks = sorted(range(chunks), key=lambda owner: rank_of(owner, chunks))

    def exchange(x):
        return lax.all_to_all(x, "mem", split_axis=0, concat_axis=0, axis_index_groups=[ranks], tiled=True)

    regional = exchange(sent)
    analysed = pl.pallas_call(
        analysis_kernel,
        out_shape=jax.ShapeDtypeStruct((chunks, per, width), jnp.float32),
        in_specs=[VMEM] * 2,
        out_specs=VMEM,
        compiler_params=params(),
        name="analysis",
    )(columns, regional)
    back = exchange(analysed)
    return pl.pallas_call(
        unpack_kernel,
        out_shape=jax.ShapeDtypeStruct((per, rows, lon), jnp.float32),
        in_specs=[VMEM],
        out_specs=VMEM,
        compiler_params=params(),
        name="unpack",
    )(back)


def solution(mesh):
    placed = (
        P("mem", "strip", None),
        P("strip", None),
        P(("strip", "mem"), None),
        P(("strip", "mem")),
        P(("strip", "mem"), None),
        P(("strip", "mem"), None),
    )
    return jax.shard_map(local, mesh=mesh, in_specs=placed, out_specs=P("mem", "strip", None), check_vma=False)
```

```python
import functools
import math

import jax
import jax.numpy as jnp
from jax import lax
from jax.experimental import pallas as pl
from jax.experimental.pallas import tpu as pltpu
from jax.sharding import PartitionSpec as P


STEPS = 4
NS_ITERS = 4
REGION_VALUES = 256

step_size = 0.05
coupling = 0.4

VMEM = pl.BlockSpec(memory_space=pltpu.VMEM)
ANY = pl.BlockSpec(memory_space=pl.ANY)
SMEM = pl.BlockSpec(memory_space=pltpu.SMEM)
GRANT = 16 * 1024 * 1024


def params():
    return pltpu.CompilerParams(vmem_limit_bytes=GRANT)


def leader_of(strip):
    return jnp.where(strip < 2, 0, 20) if not isinstance(strip, int) else 0 if strip < 2 else 20


def rank_of(owner, leader, count):
    return lax.rem(owner + count - leader, count)


def row_of(line, parity):
    return line if parity == 0 else 2 * STEPS - 1 - line


def pack_kernel(strip_ref, ens_ref, forcing_ref, cross_ref, near_ref):
    odd = lax.rem(strip_ref[0], 2)
    half = cross_ref.shape[2]
    for parity in (0, 1):

        @pl.when(odd == parity)
        def _():
            for line in range(2 * STEPS):
                message = cross_ref if line < STEPS else near_ref
                at, row = line % STEPS, row_of(line, parity)
                state, force = ens_ref[:, row, :], forcing_ref[row : row + 1, :]
                for side in range(2):
                    lons = slice(side * half, (side + 1) * half)
                    message[2 * at + side] = state[:, lons]
                    spot = side * STEPS + at
                    message[2 * STEPS, spot : spot + 1, :] = force[:, lons]


def columns_kernel(count_ref, index_ref, value_ref, precision_ref, after_ref, columns_ref):
    slots = index_ref.shape[1]
    slot = lax.broadcasted_iota(jnp.int32, (1, slots), 1)
    lines = []
    for region in range(index_ref.shape[0]):
        live = (slot < count_ref[region]).astype(jnp.float32)
        weight = precision_ref[region : region + 1, :] * live
        lines += [
            index_ref[region : region + 1, :].astype(jnp.float32),
            jnp.sqrt(weight),
            value_ref[region : region + 1, :],
            weight,
        ]
    columns_ref[...] = jnp.concatenate(lines, axis=0).T


def state_of(message, at):
    return jnp.concatenate([message[2 * at], message[2 * at + 1]], axis=1)


def force_of(message, at):
    both = [message[2 * STEPS, spot : spot + 1, :] for spot in (at, STEPS + at)]
    return jnp.concatenate(both, axis=1)


def advance(before, center, after, force):
    lon = center.shape[1]
    west = pltpu.roll(center, 1, 1)
    west2 = pltpu.roll(center, 2, 1)
    east = pltpu.roll(center, lon - 1, 1)
    return (
        center * (1.0 - step_size - 2.0 * coupling)
        + step_size * ((east - west2) * west + force)
        + coupling * (before + after)
    )


def put_line(out_ref, odd, leader, line, value):
    width = out_ref.shape[2]
    parts = value.shape[1] // width
    row = line + odd * (2 * STEPS - 1 - 2 * line)
    for part in range(parts):
        chunk = rank_of(row * parts + part, leader, out_ref.shape[0])
        out_ref[chunk] = value[:, part * width : (part + 1) * width]


def near_kernel(after_ref, own_cross_ref, own_near_ref, got_near_ref, done_ref, edge_ref, *levels):
    def start(read):
        def of(line):
            if line < STEPS:
                return read(own_cross_ref, line)
            if line < 2 * STEPS:
                return read(own_near_ref, line - STEPS)
            return read(got_near_ref, 3 * STEPS - 1 - line)

        return of

    force = start(force_of)
    read = start(state_of)
    for step in range(1, STEPS + 1):
        for line in range(step, 3 * STEPS - step):
            new = advance(read(line - 1), read(line), read(line + 1), force(line))
            if step == STEPS:
                done_ref[line - STEPS] = new
            else:
                levels[step - 1][line - step] = new
                if line < step + 2:
                    edge_ref[2 * (step - 1) + line - step] = new
        if step < STEPS:
            read = lambda line, step=step: levels[step - 1][line - step]


def cross_kernel(last, strip_ref, done_ref, own_cross_ref, got_cross_ref, edge_ref, out_ref, *levels):
    strip = strip_ref[0]
    odd = lax.rem(strip, 2)
    leader = leader_of(strip)
    kept = jnp.where(jnp.logical_or(strip == 0, strip == last), 0.0, 1.0)

    def start(read):
        return lambda line: read(own_cross_ref, line) if line >= 0 else read(got_cross_ref, -1 - line)

    for line in range(STEPS):
        put_line(out_ref, odd, leader, STEPS + line, done_ref[line])
    force = start(force_of)
    read = start(state_of)
    for step in range(1, STEPS + 1):
        first = step - STEPS
        for line in range(first, first + STEPS):
            new = advance(read(line - 1), read(line), read(line + 1), force(line))
            if line < 0:
                new = new * kept
            if step == STEPS:
                put_line(out_ref, odd, leader, line, new)
            else:
                levels[step - 1][line - first] = new
        if step < STEPS:

            def read(line, step=step, first=first):
                if line < step:
                    return levels[step - 1][line - first]
                return edge_ref[2 * (step - 1) + line - step]


NN = (((1,), (0,)), ((), ()))
NT = (((1,), (1,)), ((), ()))


def halves(x):
    high = x.astype(jnp.bfloat16)
    return high, (x - high.astype(jnp.float32)).astype(jnp.bfloat16)


def dot(a, b, dims=NN):
    return lax.dot_general(a, b, dims, preferred_element_type=jnp.float32)


def across(parts):
    high, low = parts
    return jnp.concatenate([high, low, high], axis=1)


def down(parts):
    high, low = parts
    return jnp.concatenate([high, high, low], axis=0)


def stack(*parts):
    return tuple(jnp.concatenate(p, axis=0) for p in zip(*parts))


def product(a, b):
    return dot(across(a), down(b))


def analysis_kernel(columns_ref, block_ref, out_ref):
    chunks, per, _ = block_ref.shape
    members = chunks * per
    slots = columns_ref.shape[0]
    regions = block_ref.shape[2] // REGION_VALUES
    top = members - 1.0
    columns = columns_ref[...]
    eye = (lax.broadcasted_iota(jnp.int32, (slots, slots), 0) == lax.broadcasted_iota(jnp.int32, (slots, slots), 1)).astype(jnp.float32)
    cell = lax.broadcasted_iota(jnp.int32, (slots, REGION_VALUES), 1).astype(jnp.float32)

    def begin(r):
        cells = slice(r * REGION_VALUES, (r + 1) * REGION_VALUES)
        block = block_ref[:, :, cells].reshape(members, REGION_VALUES)
        index, root, value = (columns[:, 4 * r + i : 4 * r + i + 1] for i in range(3))
        mean = jnp.sum(block, axis=0, keepdims=True) * (1.0 / members)
        spread = block - mean
        sh, sl = halves(spread)
        chosen = cell == index
        onehot = chosen.astype(jnp.bfloat16)
        observed = dot(onehot, sh, NT) + dot(onehot, sl, NT)
        obs_mean = jnp.sum(jnp.where(chosen, mean, 0.0), axis=1, keepdims=True)
        scaled = observed * root
        misfit = root * (value - obs_mean)
        gh, gl = halves(scaled)
        small = dot(jnp.concatenate([gh, gl, gh], axis=1), jnp.concatenate([gh, gh, gl], axis=1), NT)
        carried = product((gh, gl), (sh, sl))
        norm = top + jnp.sqrt(jnp.sum(small * small, keepdims=True))
        inverse = 1.0 / norm
        return dict(mean=mean, scaled=scaled, misfit=misfit, carried=carried, norm=norm, inverse=inverse, small=small)

    def iterate(s):
        inverse = s["inverse"]
        left = (top * inverse) * eye + s["small"] * inverse
        left_zero = top * inverse
        fix = 1.5 * eye - 0.5 * left
        fix_zero = 1.5 - 0.5 * left_zero
        f = halves(fix)
        square = product(f, f)
        yield 2
        mixed = square - (0.5 * left_zero) * (fix + fix_zero * eye)
        left_rest = inverse * mixed
        left = product(halves(left), halves(square))
        yield 2
        right, right_zero, rest = fix, fix_zero, (-0.5 * inverse) * eye
        left_zero = left_zero * fix_zero * fix_zero
        for repeat in range(1, NS_ITERS):
            fix = 1.5 * eye - 0.5 * left
            fix_zero = 1.5 - 0.5 * left_zero
            f = halves(fix)
            last = repeat == NS_ITERS - 1
            rows = [halves(right)] if last else [f, halves(right), halves(left_rest)]
            if repeat > 1: rows.append(halves(rest))
            got = product(stack(*rows), f)
            got = [got[i * slots : (i + 1) * slots] for i in range(len(rows))]
            yield 2
            new_rest = (got[-1] if repeat > 1 else (-0.5 * inverse) * fix) - (0.5 * right_zero) * left_rest
            if not last:
                square, right, rest_fix = got[:3]
                both = product(stack(halves(left), halves(left_rest)), halves(square))
                left = both[:slots]
                left_rest = both[slots:] - (0.5 * left_zero) * (rest_fix + fix_zero * left_rest)
                left_zero = left_zero * fix_zero * fix_zero
                yield 2
            else:
                right = got[0]
            rest = new_rest
            right_zero = right_zero * fix_zero
        s.update(right=right, right_zero=right_zero, rest=rest)

    def finish(r, s):
        cells = slice(r * REGION_VALUES, (r + 1) * REGION_VALUES)
        right, carried = s["right"], s["carried"]
        along = jnp.sum(right * s["misfit"], axis=0, keepdims=True)
        twice = jnp.sum(right * along, axis=1, keepdims=True)
        moved = jnp.sum(twice * carried, axis=0, keepdims=True) * s["inverse"]
        pushed = product(halves(s["rest"]), halves(carried))
        gain = math.sqrt(top) * lax.rsqrt(s["norm"])
        update = product(halves(s["scaled"].T * gain), halves(pushed))
        block = block_ref[:, :, cells].reshape(members, REGION_VALUES)
        keep = gain * s["right_zero"]
        result = keep * block + (s["mean"] * (1.0 - keep) + moved) + update
        out_ref[:, :, cells] = result.reshape(chunks, per, REGION_VALUES)

    states = [begin(r) for r in range(regions)]
    runs = [iterate(s) for s in states]
    while runs:
        runs = [run for run in runs if next(run, 0)]
    for r in range(regions):
        finish(r, states[r])


def unpack_kernel(strip_ref, block_ref, out_ref):
    leader = leader_of(strip_ref[0])
    rows = out_ref.shape[1]
    parts = block_ref.shape[0] // rows
    width = block_ref.shape[2]
    for row in range(rows):
        for part in range(parts):
            out_ref[:, row, part * width : (part + 1) * width] = block_ref[rank_of(row * parts + part, leader, block_ref.shape[0])]


def local(ensemble, forcing, obs_index, obs_count, obs_value, obs_precision):
    per, rows, lon = ensemble.shape
    strips = lax.axis_size("strip")
    strip = lax.axis_index("strip").astype(jnp.int32).reshape(1)
    regions, slots = obs_index.shape
    message = jax.ShapeDtypeStruct((2 * STEPS + 1, per, lon // 2), jnp.float32)

    cross, near = pl.pallas_call(
        pack_kernel,
        out_shape=(message, message),
        in_specs=[SMEM, VMEM, VMEM],
        out_specs=(VMEM, VMEM),
        compiler_params=params(),
        name="pack",
    )(strip, ensemble, forcing)
    span = [(i, i + 1) for i in range(1, strips - 1, 2)]
    span = span + [(b, a) for a, b in span]
    swap = [(i, i ^ 1) for i in range(strips)]
    got_cross = lax.ppermute(cross, "strip", span)
    got_near = lax.ppermute(near, "strip", swap)
    columns = pl.pallas_call(
        columns_kernel,
        out_shape=jax.ShapeDtypeStruct((slots, 4 * regions), jnp.float32),
        in_specs=[SMEM] + [VMEM] * 3 + [ANY],
        out_specs=VMEM,
        compiler_params=params(),
        cost_estimate=pl.CostEstimate(flops=10**7, bytes_accessed=4096, transcendentals=0),
        name="columns",
    )(obs_count, obs_index, obs_value, obs_precision, near)
    chunks = lax.axis_size("mem")
    width = rows * lon // chunks
    full = jax.ShapeDtypeStruct((chunks, per, width), jnp.float32)

    def line_slabs(count):
        return pltpu.VMEM((count, per, lon), jnp.float32)

    done, edges = pl.pallas_call(
        near_kernel,
        out_shape=tuple(jax.ShapeDtypeStruct((count, per, lon), jnp.float32) for count in (STEPS, 2 * (STEPS - 1))),
        in_specs=[ANY] + [VMEM] * 3,
        out_specs=(VMEM, VMEM),
        scratch_shapes=[line_slabs(3 * STEPS - 2 * step) for step in range(1, STEPS)],
        compiler_params=params(),
        cost_estimate=pl.CostEstimate(flops=10**8, bytes_accessed=4096, transcendentals=0),
        name="forecast_near",
    )(columns, cross, near, got_near)
    sent = pl.pallas_call(
        functools.partial(cross_kernel, strips - 1),
        out_shape=full,
        in_specs=[SMEM] + [VMEM] * 4,
        out_specs=VMEM,
        scratch_shapes=[line_slabs(STEPS) for _ in range(1, STEPS)],
        compiler_params=params(),
        name="forecast_cross",
    )(strip, done, cross, got_cross, edges)
    groups = [
        [i * chunks + (leader_of(i) + rank) % chunks for rank in range(chunks)] for i in range(strips)
    ]

    def exchange(x):
        return lax.all_to_all(x, ("strip", "mem"), split_axis=0, concat_axis=0, axis_index_groups=groups, tiled=True)

    regional = exchange(sent)
    analysed = pl.pallas_call(
        analysis_kernel,
        out_shape=jax.ShapeDtypeStruct((chunks, per, width), jnp.float32),
        in_specs=[VMEM] * 2,
        out_specs=VMEM,
        compiler_params=params(),
        name="analysis",
    )(columns, regional)
    back = exchange(analysed)
    return pl.pallas_call(
        unpack_kernel,
        out_shape=jax.ShapeDtypeStruct((per, rows, lon), jnp.float32),
        in_specs=[SMEM, VMEM],
        out_specs=VMEM,
        compiler_params=params(),
        name="unpack",
    )(strip, back)


def solution(mesh):
    placed = (
        P("mem", "strip", None),
        P("strip", None),
        P(("strip", "mem"), None),
        P(("strip", "mem")),
        P(("strip", "mem"), None),
        P(("strip", "mem"), None),
    )
    return jax.shard_map(local, mesh=mesh, in_specs=placed, out_specs=P("mem", "strip", None), check_vma=False)
```

```python
import functools
import math

import jax
import jax.numpy as jnp
from jax import lax
from jax.experimental import pallas as pl
from jax.experimental.pallas import tpu as pltpu
from jax.sharding import PartitionSpec as P


STEPS = 4
NS_ITERS = 4
REGION_VALUES = 256

step_size = 0.05
coupling = 0.4

VMEM = pl.BlockSpec(memory_space=pltpu.VMEM)
ANY = pl.BlockSpec(memory_space=pl.ANY)
SMEM = pl.BlockSpec(memory_space=pltpu.SMEM)
GRANT = 16 * 1024 * 1024


def params():
    return pltpu.CompilerParams(vmem_limit_bytes=GRANT)


def leader_of(strip):
    return jnp.where(strip < 2, 0, 20) if not isinstance(strip, int) else 0 if strip < 2 else 20


def rank_of(owner, leader, count):
    return lax.rem(owner + count - leader, count)


def row_of(line, parity):
    return line if parity == 0 else 2 * STEPS - 1 - line


def pack_kernel(strip_ref, ens_ref, forcing_ref, cross_ref, near_ref):
    odd = lax.rem(strip_ref[0], 2)
    half = cross_ref.shape[2]
    for parity in (0, 1):

        @pl.when(odd == parity)
        def _():
            for line in range(2 * STEPS):
                inner = line < STEPS
                message, at = (cross_ref, line) if inner else (near_ref, 2 * STEPS - 1 - line)
                row = row_of(line, parity)
                state, force = ens_ref[:, row, :], forcing_ref[row : row + 1, :]
                for side in range(2):
                    lons = slice(side * half, (side + 1) * half)
                    message[2 * at + side] = state[:, lons]
                    spot = side * STEPS + at
                    message[2 * STEPS, spot : spot + 1, :] = force[:, lons]


def state_of(message, at):
    return jnp.concatenate([message[2 * at], message[2 * at + 1]], axis=1)


def force_of(message, at):
    both = [message[2 * STEPS, spot : spot + 1, :] for spot in (at, STEPS + at)]
    return jnp.concatenate(both, axis=1)


def advance(before, center, after, force):
    lon = center.shape[1]
    west = pltpu.roll(center, 1, 1)
    west2 = pltpu.roll(center, 2, 1)
    east = pltpu.roll(center, lon - 1, 1)
    return (
        center * (1.0 - step_size - 2.0 * coupling)
        + step_size * ((east - west2) * west + force)
        + coupling * (before + after)
    )


def put_line(out_ref, odd, leader, line, value):
    width = out_ref.shape[2]
    parts = value.shape[1] // width
    row = line + odd * (2 * STEPS - 1 - 2 * line)
    for part in range(parts):
        chunk = rank_of(row * parts + part, leader, out_ref.shape[0])
        out_ref[chunk] = value[:, part * width : (part + 1) * width]


def own_kernel(
    count_ref, index_ref, value_ref, precision_ref, own_cross_ref, own_near_ref,
    columns_ref, cross_edge_ref, near_edge_ref, *levels
):
    slots = index_ref.shape[1]
    slot = lax.broadcasted_iota(jnp.int32, (1, slots), 1)
    lines = []
    for region in range(index_ref.shape[0]):
        live = (slot < count_ref[region]).astype(jnp.float32)
        weight = precision_ref[region : region + 1, :] * live
        lines += [
            index_ref[region : region + 1, :].astype(jnp.float32),
            jnp.sqrt(weight),
            value_ref[region : region + 1, :],
            weight,
        ]
    columns_ref[...] = jnp.concatenate(lines, axis=0).T

    def start(read):
        return lambda line: read(own_cross_ref, line) if line < STEPS else read(own_near_ref, 2 * STEPS - 1 - line)

    force = start(force_of)
    read = start(state_of)
    for step in range(1, STEPS):
        last = 2 * STEPS - 1 - step
        for line in range(step, last + 1):
            new = advance(read(line - 1), read(line), read(line + 1), force(line))
            levels[step - 1][line - step] = new
            for edge_ref, at in ((cross_edge_ref, line - step), (near_edge_ref, last - line)):
                if at < 2:
                    edge_ref[2 * (step - 1) + at] = new
        read = lambda line, step=step: levels[step - 1][line - step]


def border_lines(own_ref, got_ref, edge_ref, levels, kept, put):
    def start(read):
        return lambda at: read(own_ref, at) if at >= 0 else read(got_ref, -1 - at)

    force = start(force_of)
    read = start(state_of)
    for step in range(1, STEPS + 1):
        first = step - STEPS
        for at in range(first, first + STEPS):
            new = advance(read(at - 1), read(at), read(at + 1), force(at))
            if at < 0 and kept is not None:
                new = new * kept
            if step == STEPS:
                put(at, new)
            else:
                levels[step - 1][at - first] = new
        if step < STEPS:

            def read(at, step=step, first=first):
                if at < step:
                    return levels[step - 1][at - first]
                return edge_ref[2 * (step - 1) + at - step]


def near_kernel(own_ref, got_ref, edge_ref, done_ref, *levels):
    def put(at, value):
        done_ref[at] = value

    border_lines(own_ref, got_ref, edge_ref, levels, None, put)


def cross_kernel(last, strip_ref, columns_ref, done_ref, own_ref, got_ref, edge_ref, out_ref, *levels):
    strip = strip_ref[0]
    odd = lax.rem(strip, 2)
    leader = leader_of(strip)
    for at in range(STEPS):
        put_line(out_ref, odd, leader, 2 * STEPS - 1 - at, done_ref[at])
    kept = jnp.where(jnp.logical_or(strip == 0, strip == last), 0.0, 1.0)
    put = lambda at, value: put_line(out_ref, odd, leader, at, value)
    border_lines(own_ref, got_ref, edge_ref, levels, kept, put)


NN = (((1,), (0,)), ((), ()))
NT = (((1,), (1,)), ((), ()))


def halves(x):
    high = x.astype(jnp.bfloat16)
    return high, (x - high.astype(jnp.float32)).astype(jnp.bfloat16)


def dot(a, b, dims=NN):
    return lax.dot_general(a, b, dims, preferred_element_type=jnp.float32)


def across(parts):
    high, low = parts
    return jnp.concatenate([high, low, high], axis=1)


def down(parts):
    high, low = parts
    return jnp.concatenate([high, high, low], axis=0)


def stack(*parts):
    return tuple(jnp.concatenate(p, axis=0) for p in zip(*parts))


def product(a, b):
    return dot(across(a), down(b))


def analysis_kernel(columns_ref, block_ref, out_ref):
    chunks, per, _ = block_ref.shape
    members = chunks * per
    slots = columns_ref.shape[0]
    regions = block_ref.shape[2] // REGION_VALUES
    top = members - 1.0
    columns = columns_ref[...]
    eye = (lax.broadcasted_iota(jnp.int32, (slots, slots), 0) == lax.broadcasted_iota(jnp.int32, (slots, slots), 1)).astype(jnp.float32)
    cell = lax.broadcasted_iota(jnp.int32, (slots, REGION_VALUES), 1).astype(jnp.float32)

    def begin(r):
        cells = slice(r * REGION_VALUES, (r + 1) * REGION_VALUES)
        block = block_ref[:, :, cells].reshape(members, REGION_VALUES)
        index, root, value = (columns[:, 4 * r + i : 4 * r + i + 1] for i in range(3))
        mean = jnp.sum(block, axis=0, keepdims=True) * (1.0 / members)
        spread = block - mean
        sh, sl = halves(spread)
        chosen = cell == index
        onehot = chosen.astype(jnp.bfloat16)
        observed = dot(onehot, sh, NT) + dot(onehot, sl, NT)
        obs_mean = jnp.sum(jnp.where(chosen, mean, 0.0), axis=1, keepdims=True)
        scaled = observed * root
        misfit = root * (value - obs_mean)
        gh, gl = halves(scaled)
        small = dot(jnp.concatenate([gh, gl, gh], axis=1), jnp.concatenate([gh, gh, gl], axis=1), NT)
        carried = product((gh, gl), (sh, sl))
        norm = top + jnp.sqrt(jnp.sum(small * small, keepdims=True))
        inverse = 1.0 / norm
        return dict(mean=mean, scaled=scaled, misfit=misfit, carried=carried, norm=norm, inverse=inverse, small=small)

    def iterate(s):
        inverse = s["inverse"]
        left = (top * inverse) * eye + s["small"] * inverse
        left_zero = top * inverse
        fix = 1.5 * eye - 0.5 * left
        fix_zero = 1.5 - 0.5 * left_zero
        f = halves(fix)
        square = product(f, f)
        yield 2
        mixed = square - (0.5 * left_zero) * (fix + fix_zero * eye)
        left_rest = inverse * mixed
        left = product(halves(left), halves(square))
        yield 2
        right, right_zero, rest = fix, fix_zero, (-0.5 * inverse) * eye
        left_zero = left_zero * fix_zero * fix_zero
        for repeat in range(1, NS_ITERS):
            fix = 1.5 * eye - 0.5 * left
            fix_zero = 1.5 - 0.5 * left_zero
            f = halves(fix)
            last = repeat == NS_ITERS - 1
            rows = [halves(right)] if last else [f, halves(right), halves(left_rest)]
            if repeat > 1: rows.append(halves(rest))
            got = product(stack(*rows), f)
            got = [got[i * slots : (i + 1) * slots] for i in range(len(rows))]
            yield 2
            new_rest = (got[-1] if repeat > 1 else (-0.5 * inverse) * fix) - (0.5 * right_zero) * left_rest
            if not last:
                square, right, rest_fix = got[:3]
                both = product(stack(halves(left), halves(left_rest)), halves(square))
                left = both[:slots]
                left_rest = both[slots:] - (0.5 * left_zero) * (rest_fix + fix_zero * left_rest)
                left_zero = left_zero * fix_zero * fix_zero
                yield 2
            else:
                right = got[0]
            rest = new_rest
            right_zero = right_zero * fix_zero
        s.update(right=right, right_zero=right_zero, rest=rest)

    def finish(r, s):
        cells = slice(r * REGION_VALUES, (r + 1) * REGION_VALUES)
        right, carried = s["right"], s["carried"]
        along = jnp.sum(right * s["misfit"], axis=0, keepdims=True)
        twice = jnp.sum(right * along, axis=1, keepdims=True)
        moved = jnp.sum(twice * carried, axis=0, keepdims=True) * s["inverse"]
        pushed = product(halves(s["rest"]), halves(carried))
        gain = math.sqrt(top) * lax.rsqrt(s["norm"])
        update = product(halves(s["scaled"].T * gain), halves(pushed))
        block = block_ref[:, :, cells].reshape(members, REGION_VALUES)
        keep = gain * s["right_zero"]
        result = keep * block + (s["mean"] * (1.0 - keep) + moved) + update
        out_ref[:, :, cells] = result.reshape(chunks, per, REGION_VALUES)

    states = [begin(r) for r in range(regions)]
    runs = [iterate(s) for s in states]
    while runs:
        runs = [run for run in runs if next(run, 0)]
    for r in range(regions):
        finish(r, states[r])


def unpack_kernel(strip_ref, block_ref, out_ref):
    leader = leader_of(strip_ref[0])
    rows = out_ref.shape[1]
    parts = block_ref.shape[0] // rows
    width = block_ref.shape[2]
    for row in range(rows):
        for part in range(parts):
            out_ref[:, row, part * width : (part + 1) * width] = block_ref[rank_of(row * parts + part, leader, block_ref.shape[0])]


def local(ensemble, forcing, obs_index, obs_count, obs_value, obs_precision):
    per, rows, lon = ensemble.shape
    strips = lax.axis_size("strip")
    strip = lax.axis_index("strip").astype(jnp.int32).reshape(1)
    regions, slots = obs_index.shape
    message = jax.ShapeDtypeStruct((2 * STEPS + 1, per, lon // 2), jnp.float32)

    cross, near = pl.pallas_call(
        pack_kernel,
        out_shape=(message, message),
        in_specs=[SMEM, VMEM, VMEM],
        out_specs=(VMEM, VMEM),
        compiler_params=params(),
        name="pack",
    )(strip, ensemble, forcing)
    span = [(i, i + 1) for i in range(1, strips - 1, 2)]
    span = span + [(b, a) for a, b in span]
    swap = [(i, i ^ 1) for i in range(strips)]
    got_cross = lax.ppermute(cross, "strip", span)
    got_near = lax.ppermute(near, "strip", swap)

    def line_slabs(count):
        return pltpu.VMEM((count, per, lon), jnp.float32)

    edges = jax.ShapeDtypeStruct((2 * (STEPS - 1), per, lon), jnp.float32)
    border_levels = [line_slabs(STEPS) for _ in range(1, STEPS)]
    columns, cross_edge, near_edge = pl.pallas_call(
        own_kernel,
        out_shape=(jax.ShapeDtypeStruct((slots, 4 * regions), jnp.float32), edges, edges),
        in_specs=[SMEM] + [VMEM] * 5,
        out_specs=(VMEM,) * 3,
        scratch_shapes=[line_slabs(2 * STEPS - 2 * step) for step in range(1, STEPS)],
        compiler_params=params(),
        cost_estimate=pl.CostEstimate(flops=10**8, bytes_accessed=4096, transcendentals=0),
        name="forecast_own",
    )(obs_count, obs_index, obs_value, obs_precision, cross, near)
    chunks = lax.axis_size("mem")
    width = rows * lon // chunks
    full = jax.ShapeDtypeStruct((chunks, per, width), jnp.float32)

    done = pl.pallas_call(
        near_kernel,
        out_shape=jax.ShapeDtypeStruct((STEPS, per, lon), jnp.float32),
        in_specs=[VMEM] * 3,
        out_specs=VMEM,
        scratch_shapes=border_levels,
        compiler_params=params(),
        cost_estimate=pl.CostEstimate(flops=10**8, bytes_accessed=4096, transcendentals=0),
        name="forecast_near",
    )(near, got_near, near_edge)
    sent = pl.pallas_call(
        functools.partial(cross_kernel, strips - 1),
        out_shape=full,
        in_specs=[SMEM, ANY] + [VMEM] * 4,
        out_specs=VMEM,
        scratch_shapes=border_levels,
        compiler_params=params(),
        name="forecast_cross",
    )(strip, columns, done, cross, got_cross, cross_edge)
    groups = [
        [i * chunks + (leader_of(i) + rank) % chunks for rank in range(chunks)] for i in range(strips)
    ]

    def exchange(x):
        return lax.all_to_all(x, ("strip", "mem"), split_axis=0, concat_axis=0, axis_index_groups=groups, tiled=True)

    regional = exchange(sent)
    analysed = pl.pallas_call(
        analysis_kernel,
        out_shape=jax.ShapeDtypeStruct((chunks, per, width), jnp.float32),
        in_specs=[VMEM] * 2,
        out_specs=VMEM,
        compiler_params=params(),
        name="analysis",
    )(columns, regional)
    back = exchange(analysed)
    return pl.pallas_call(
        unpack_kernel,
        out_shape=jax.ShapeDtypeStruct((per, rows, lon), jnp.float32),
        in_specs=[SMEM, VMEM],
        out_specs=VMEM,
        compiler_params=params(),
        name="unpack",
    )(strip, back)


def solution(mesh):
    placed = (
        P("mem", "strip", None),
        P("strip", None),
        P(("strip", "mem"), None),
        P(("strip", "mem")),
        P(("strip", "mem"), None),
        P(("strip", "mem"), None),
    )
    return jax.shard_map(local, mesh=mesh, in_specs=placed, out_specs=P("mem", "strip", None), check_vma=False)
```

```python
import functools
import math

import jax
import jax.numpy as jnp
from jax import lax
from jax.experimental import pallas as pl
from jax.experimental.pallas import tpu as pltpu
from jax.sharding import PartitionSpec as P


STEPS = 4
NS_ITERS = 4
REGION_VALUES = 256

step_size = 0.05
coupling = 0.4

VMEM = pl.BlockSpec(memory_space=pltpu.VMEM)
ANY = pl.BlockSpec(memory_space=pl.ANY)
SMEM = pl.BlockSpec(memory_space=pltpu.SMEM)
GRANT = 16 * 1024 * 1024


def params():
    return pltpu.CompilerParams(vmem_limit_bytes=GRANT)


def leader_of(strip):
    return jnp.where(strip < 2, 0, 20) if not isinstance(strip, int) else 0 if strip < 2 else 20


def rank_of(owner, leader, count):
    return lax.rem(owner + count - leader, count)


def row_of(line, parity):
    return line if parity == 0 else 2 * STEPS - 1 - line


def pack_kernel(strip_ref, ens_ref, forcing_ref, cross_ref, near_ref, held_ref, force_ref, arrived):
    odd = lax.rem(strip_ref[0], 2)
    half = cross_ref.shape[2]
    lons = [pl.ds(side * half, half) for side in range(2)]
    copies = [pltpu.make_async_copy(forcing_ref, force_ref, arrived.at[2])]
    copies += [
        pltpu.make_async_copy(ens_ref.at[:, :, lons[side]], held_ref.at[side], arrived.at[side])
        for side in range(2)
    ]
    for copy in copies:
        copy.start()
    copies[0].wait()
    for side in range(2):
        copies[1 + side].wait()
        for parity in (0, 1):

            @pl.when(odd == parity)
            def _():
                for line in range(2 * STEPS):
                    inner = line < STEPS
                    message, at = (cross_ref, line) if inner else (near_ref, 2 * STEPS - 1 - line)
                    row, spot = row_of(line, parity), side * STEPS + at
                    message[2 * at + side] = held_ref[side, :, row, :]
                    message[2 * STEPS, spot : spot + 1, :] = force_ref[row : row + 1, lons[side]]


def state_of(message, at):
    if isinstance(message, tuple):
        return state_of(message[0], at) + state_of(message[1], at)
    return jnp.concatenate([message[2 * at], message[2 * at + 1]], axis=1)


def force_of(message, at):
    if isinstance(message, tuple):
        return force_of(message[0], at) + force_of(message[1], at)
    both = [message[2 * STEPS, spot : spot + 1, :] for spot in (at, STEPS + at)]
    return jnp.concatenate(both, axis=1)


def advance(before, center, after, force):
    lon = center.shape[1]
    west = pltpu.roll(center, 1, 1)
    west2 = pltpu.roll(center, 2, 1)
    east = pltpu.roll(center, lon - 1, 1)
    return (
        center * (1.0 - step_size - 2.0 * coupling)
        + step_size * ((east - west2) * west + force)
        + coupling * (before + after)
    )


def put_line(out_ref, odd, leader, line, value):
    width = out_ref.shape[2]
    parts = value.shape[1] // width
    row = line + odd * (2 * STEPS - 1 - 2 * line)
    for part in range(parts):
        chunk = rank_of(row * parts + part, leader, out_ref.shape[0])
        out_ref[chunk] = value[:, part * width : (part + 1) * width]


def own_kernel(
    count_ref, index_ref, value_ref, precision_ref, own_cross_ref, own_near_ref,
    columns_ref, cross_edge_ref, near_edge_ref, *levels
):
    slots = index_ref.shape[1]
    slot = lax.broadcasted_iota(jnp.int32, (1, slots), 1)
    lines = []
    for region in range(index_ref.shape[0]):
        live = (slot < count_ref[region]).astype(jnp.float32)
        weight = precision_ref[region : region + 1, :] * live
        lines += [
            index_ref[region : region + 1, :].astype(jnp.float32),
            jnp.sqrt(weight),
            value_ref[region : region + 1, :],
            weight,
        ]
    columns_ref[...] = jnp.concatenate(lines, axis=0).T

    def start(read):
        return lambda line: read(own_cross_ref, line) if line < STEPS else read(own_near_ref, 2 * STEPS - 1 - line)

    force = start(force_of)
    read = start(state_of)
    for step in range(1, STEPS):
        last = 2 * STEPS - 1 - step
        for line in range(step, last + 1):
            new = advance(read(line - 1), read(line), read(line + 1), force(line))
            levels[step - 1][line - step] = new
            for edge_ref, at in ((cross_edge_ref, line - step), (near_edge_ref, last - line)):
                if at < 2:
                    edge_ref[2 * (step - 1) + at] = new
        read = lambda line, step=step: levels[step - 1][line - step]


def border_lines(own_ref, got_ref, edge_ref, levels, kept, put):
    def start(read):
        return lambda at: read(own_ref, at) if at >= 0 else read(got_ref, -1 - at)

    force = start(force_of)
    read = start(state_of)
    for step in range(1, STEPS + 1):
        first = step - STEPS
        for at in range(first, first + STEPS):
            new = advance(read(at - 1), read(at), read(at + 1), force(at))
            if at < 0 and kept is not None:
                new = new * kept
            if step == STEPS:
                put(at, new)
            else:
                levels[step - 1][at - first] = new
        if step < STEPS:

            def read(at, step=step, first=first):
                if at < step:
                    return levels[step - 1][at - first]
                return edge_ref[2 * (step - 1) + at - step]


def near_kernel(own_ref, got_ref, edge_ref, done_ref, *levels):
    def put(at, value):
        done_ref[at] = value

    border_lines(own_ref, got_ref, edge_ref, levels, None, put)


def cross_kernel(last, strip_ref, columns_ref, done_ref, own_ref, got_early_ref, got_late_ref, edge_ref, out_ref, *levels):
    strip = strip_ref[0]
    odd = lax.rem(strip, 2)
    leader = leader_of(strip)
    for at in range(STEPS):
        put_line(out_ref, odd, leader, 2 * STEPS - 1 - at, done_ref[at])
    kept = jnp.where(jnp.logical_or(strip == 0, strip == last), 0.0, 1.0)
    put = lambda at, value: put_line(out_ref, odd, leader, at, value)
    border_lines(own_ref, (got_early_ref, got_late_ref), edge_ref, levels, kept, put)


NN = (((1,), (0,)), ((), ()))
NT = (((1,), (1,)), ((), ()))


def halves(x):
    high = x.astype(jnp.bfloat16)
    return high, (x - high.astype(jnp.float32)).astype(jnp.bfloat16)


def dot(a, b, dims=NN):
    return lax.dot_general(a, b, dims, preferred_element_type=jnp.float32)


def across(parts):
    high, low = parts
    return jnp.concatenate([high, low, high], axis=1)


def down(parts):
    high, low = parts
    return jnp.concatenate([high, high, low], axis=0)


def stack(*parts):
    return tuple(jnp.concatenate(p, axis=0) for p in zip(*parts))


def product(a, b):
    return dot(across(a), down(b))


def analysis_kernel(columns_ref, block_ref, out_ref):
    chunks, per, _ = block_ref.shape
    members = chunks * per
    slots = columns_ref.shape[0]
    regions = block_ref.shape[2] // REGION_VALUES
    top = members - 1.0
    columns = columns_ref[...]
    eye = (lax.broadcasted_iota(jnp.int32, (slots, slots), 0) == lax.broadcasted_iota(jnp.int32, (slots, slots), 1)).astype(jnp.float32)
    cell = lax.broadcasted_iota(jnp.int32, (slots, REGION_VALUES), 1).astype(jnp.float32)

    def begin(r):
        cells = slice(r * REGION_VALUES, (r + 1) * REGION_VALUES)
        block = block_ref[:, :, cells].reshape(members, REGION_VALUES)
        index, root, value = (columns[:, 4 * r + i : 4 * r + i + 1] for i in range(3))
        mean = jnp.sum(block, axis=0, keepdims=True) * (1.0 / members)
        spread = block - mean
        sh, sl = halves(spread)
        chosen = cell == index
        onehot = chosen.astype(jnp.bfloat16)
        observed = dot(onehot, sh, NT) + dot(onehot, sl, NT)
        obs_mean = jnp.sum(jnp.where(chosen, mean, 0.0), axis=1, keepdims=True)
        scaled = observed * root
        misfit = root * (value - obs_mean)
        gh, gl = halves(scaled)
        small = dot(jnp.concatenate([gh, gl, gh], axis=1), jnp.concatenate([gh, gh, gl], axis=1), NT)
        carried = product((gh, gl), (sh, sl))
        norm = top + jnp.sqrt(jnp.sum(small * small, keepdims=True))
        inverse = 1.0 / norm
        return dict(mean=mean, scaled=scaled, misfit=misfit, carried=carried, norm=norm, inverse=inverse, small=small)

    def iterate(s):
        inverse = s["inverse"]
        left = (top * inverse) * eye + s["small"] * inverse
        left_zero = top * inverse
        fix = 1.5 * eye - 0.5 * left
        fix_zero = 1.5 - 0.5 * left_zero
        f = halves(fix)
        square = product(f, f)
        yield 2
        mixed = square - (0.5 * left_zero) * (fix + fix_zero * eye)
        left_rest = inverse * mixed
        left = product(halves(left), halves(square))
        yield 2
        right, right_zero, rest = fix, fix_zero, (-0.5 * inverse) * eye
        left_zero = left_zero * fix_zero * fix_zero
        for repeat in range(1, NS_ITERS):
            fix = 1.5 * eye - 0.5 * left
            fix_zero = 1.5 - 0.5 * left_zero
            f = halves(fix)
            last = repeat == NS_ITERS - 1
            rows = [halves(right)] if last else [f, halves(right), halves(left_rest)]
            if repeat > 1: rows.append(halves(rest))
            got = product(stack(*rows), f)
            got = [got[i * slots : (i + 1) * slots] for i in range(len(rows))]
            yield 2
            new_rest = (got[-1] if repeat > 1 else (-0.5 * inverse) * fix) - (0.5 * right_zero) * left_rest
            if not last:
                square, right, rest_fix = got[:3]
                both = product(stack(halves(left), halves(left_rest)), halves(square))
                left = both[:slots]
                left_rest = both[slots:] - (0.5 * left_zero) * (rest_fix + fix_zero * left_rest)
                left_zero = left_zero * fix_zero * fix_zero
                yield 2
            else:
                right = got[0]
            rest = new_rest
            right_zero = right_zero * fix_zero
        s.update(right=right, right_zero=right_zero, rest=rest)

    def finish(r, s):
        cells = slice(r * REGION_VALUES, (r + 1) * REGION_VALUES)
        right, carried = s["right"], s["carried"]
        along = jnp.sum(right * s["misfit"], axis=0, keepdims=True)
        twice = jnp.sum(right * along, axis=1, keepdims=True)
        moved = jnp.sum(twice * carried, axis=0, keepdims=True) * s["inverse"]
        pushed = product(halves(s["rest"]), halves(carried))
        gain = math.sqrt(top) * lax.rsqrt(s["norm"])
        update = product(halves(s["scaled"].T * gain), halves(pushed))
        block = block_ref[:, :, cells].reshape(members, REGION_VALUES)
        keep = gain * s["right_zero"]
        result = keep * block + (s["mean"] * (1.0 - keep) + moved) + update
        out_ref[:, :, cells] = result.reshape(chunks, per, REGION_VALUES)

    states = [begin(r) for r in range(regions)]
    runs = [iterate(s) for s in states]
    while runs:
        runs = [run for run in runs if next(run, 0)]
    for r in range(regions):
        finish(r, states[r])


def unpack_kernel(strip_ref, block_ref, out_ref):
    leader = leader_of(strip_ref[0])
    rows = out_ref.shape[1]
    parts = block_ref.shape[0] // rows
    width = block_ref.shape[2]
    for row in range(rows):
        for part in range(parts):
            out_ref[:, row, part * width : (part + 1) * width] = block_ref[rank_of(row * parts + part, leader, block_ref.shape[0])]


def local(ensemble, forcing, obs_index, obs_count, obs_value, obs_precision):
    per, rows, lon = ensemble.shape
    strips = lax.axis_size("strip")
    strip = lax.axis_index("strip").astype(jnp.int32).reshape(1)
    regions, slots = obs_index.shape
    message = jax.ShapeDtypeStruct((2 * STEPS + 1, per, lon // 2), jnp.float32)

    cross, near = pl.pallas_call(
        pack_kernel,
        out_shape=(message, message),
        in_specs=[SMEM, ANY, ANY],
        out_specs=(VMEM, VMEM),
        scratch_shapes=[
            pltpu.VMEM((2, per, rows, lon // 2), jnp.float32),
            pltpu.VMEM((rows, lon), jnp.float32),
            pltpu.SemaphoreType.DMA((3,)),
        ],
        compiler_params=params(),
        name="pack",
    )(strip, *(pltpu.with_memory_space_constraint(x, pltpu.HBM) for x in (ensemble, forcing)))

    def swap(message, lows):
        pairs = [(i, i + 1) for i in lows]
        return lax.ppermute(message, "strip", pairs + [(b, a) for a, b in pairs])

    got_early = swap(cross, range(1, strips - 1, 4))
    got_near = swap(near, range(0, strips, 2))
    got_late = swap(cross, range(3, strips - 1, 4))

    def line_slabs(count):
        return pltpu.VMEM((count, per, lon), jnp.float32)

    edges = jax.ShapeDtypeStruct((2 * (STEPS - 1), per, lon), jnp.float32)
    border_levels = [line_slabs(STEPS) for _ in range(1, STEPS)]
    columns, cross_edge, near_edge = pl.pallas_call(
        own_kernel,
        out_shape=(jax.ShapeDtypeStruct((slots, 4 * regions), jnp.float32), edges, edges),
        in_specs=[SMEM] + [VMEM] * 5,
        out_specs=(VMEM,) * 3,
        scratch_shapes=[line_slabs(2 * STEPS - 2 * step) for step in range(1, STEPS)],
        compiler_params=params(),
        cost_estimate=pl.CostEstimate(flops=10**8, bytes_accessed=4096, transcendentals=0),
        name="forecast_own",
    )(obs_count, obs_index, obs_value, obs_precision, cross, near)
    chunks = lax.axis_size("mem")
    width = rows * lon // chunks
    full = jax.ShapeDtypeStruct((chunks, per, width), jnp.float32)

    done = pl.pallas_call(
        near_kernel,
        out_shape=jax.ShapeDtypeStruct((STEPS, per, lon), jnp.float32),
        in_specs=[VMEM] * 3,
        out_specs=VMEM,
        scratch_shapes=border_levels,
        compiler_params=params(),
        cost_estimate=pl.CostEstimate(flops=10**8, bytes_accessed=4096, transcendentals=0),
        name="forecast_near",
    )(near, got_near, near_edge)
    sent = pl.pallas_call(
        functools.partial(cross_kernel, strips - 1),
        out_shape=full,
        in_specs=[SMEM, ANY] + [VMEM] * 5,
        out_specs=VMEM,
        scratch_shapes=border_levels,
        compiler_params=params(),
        name="forecast_cross",
    )(strip, columns, done, cross, got_early, got_late, cross_edge)
    groups = [
        [i * chunks + (leader_of(i) + rank) % chunks for rank in range(chunks)] for i in range(strips)
    ]

    def exchange(x):
        return lax.all_to_all(x, ("strip", "mem"), split_axis=0, concat_axis=0, axis_index_groups=groups, tiled=True)

    regional = exchange(sent)
    analysed = pl.pallas_call(
        analysis_kernel,
        out_shape=jax.ShapeDtypeStruct((chunks, per, width), jnp.float32),
        in_specs=[VMEM] * 2,
        out_specs=VMEM,
        compiler_params=params(),
        name="analysis",
    )(columns, regional)
    back = exchange(analysed)
    return pl.pallas_call(
        unpack_kernel,
        out_shape=jax.ShapeDtypeStruct((per, rows, lon), jnp.float32),
        in_specs=[SMEM, VMEM],
        out_specs=VMEM,
        compiler_params=params(),
        name="unpack",
    )(strip, back)


def solution(mesh):
    placed = (
        P("mem", "strip", None),
        P("strip", None),
        P(("strip", "mem"), None),
        P(("strip", "mem")),
        P(("strip", "mem"), None),
        P(("strip", "mem"), None),
    )
    return jax.shard_map(local, mesh=mesh, in_specs=placed, out_specs=P("mem", "strip", None), check_vma=False)
```

```python
import functools
import math

import jax
import jax.numpy as jnp
from jax import lax
from jax.experimental import pallas as pl
from jax.experimental.pallas import tpu as pltpu
from jax.sharding import PartitionSpec as P


STEPS = 4
NS_ITERS = 4
REGION_VALUES = 256

step_size = 0.05
coupling = 0.4

VMEM = pl.BlockSpec(memory_space=pltpu.VMEM)
ANY = pl.BlockSpec(memory_space=pl.ANY)
SMEM = pl.BlockSpec(memory_space=pltpu.SMEM)
GRANT = 16 * 1024 * 1024


def params():
    return pltpu.CompilerParams(vmem_limit_bytes=GRANT)


def leader_of(strip):
    return jnp.where(strip < 2, 0, 20) if not isinstance(strip, int) else 0 if strip < 2 else 20


def rank_of(owner, leader, count):
    return lax.rem(owner + count - leader, count)


def row_of(line, parity):
    return line if parity == 0 else 2 * STEPS - 1 - line


def pack_kernel(strip_ref, ens_ref, forcing_ref, cross_ref, near_ref, held_ref, force_ref, arrived):
    odd = lax.rem(strip_ref[0], 2)
    half = cross_ref.shape[2]
    lons = [pl.ds(side * half, half) for side in range(2)]
    copies = [pltpu.make_async_copy(forcing_ref, force_ref, arrived.at[2])]
    copies += [
        pltpu.make_async_copy(ens_ref.at[:, :, lons[side]], held_ref.at[side], arrived.at[side])
        for side in range(2)
    ]
    for copy in copies:
        copy.start()
    copies[0].wait()
    for side in range(2):
        copies[1 + side].wait()
        for parity in (0, 1):

            @pl.when(odd == parity)
            def _():
                for line in range(2 * STEPS):
                    inner = line < STEPS
                    message, at = (cross_ref, line) if inner else (near_ref, 2 * STEPS - 1 - line)
                    row, spot = row_of(line, parity), side * STEPS + at
                    message[2 * at + side] = held_ref[side, :, row, :]
                    message[2 * STEPS, spot : spot + 1, :] = force_ref[row : row + 1, lons[side]]


def state_of(message, at):
    return jnp.concatenate([message[2 * at], message[2 * at + 1]], axis=1)


def force_of(message, at):
    both = [message[2 * STEPS, spot : spot + 1, :] for spot in (at, STEPS + at)]
    return jnp.concatenate(both, axis=1)


def advance(before, center, after, force):
    lon = center.shape[1]
    west = pltpu.roll(center, 1, 1)
    west2 = pltpu.roll(center, 2, 1)
    east = pltpu.roll(center, lon - 1, 1)
    return (
        center * (1.0 - step_size - 2.0 * coupling)
        + step_size * ((east - west2) * west + force)
        + coupling * (before + after)
    )


def put_line(out_ref, odd, leader, line, value):
    width = out_ref.shape[2]
    parts = value.shape[1] // width
    row = line + odd * (2 * STEPS - 1 - 2 * line)
    for part in range(parts):
        chunk = rank_of(row * parts + part, leader, out_ref.shape[0])
        out_ref[chunk] = value[:, part * width : (part + 1) * width]


def own_kernel(
    count_ref, index_ref, value_ref, precision_ref, own_cross_ref, own_near_ref,
    columns_ref, cross_edge_ref, near_edge_ref, *levels
):
    slots = index_ref.shape[1]
    slot = lax.broadcasted_iota(jnp.int32, (1, slots), 1)
    lines = []
    for region in range(index_ref.shape[0]):
        live = (slot < count_ref[region]).astype(jnp.float32)
        weight = precision_ref[region : region + 1, :] * live
        lines += [
            index_ref[region : region + 1, :].astype(jnp.float32),
            jnp.sqrt(weight),
            value_ref[region : region + 1, :],
            weight,
        ]
    columns_ref[...] = jnp.concatenate(lines, axis=0).T

    def start(read):
        return lambda line: read(own_cross_ref, line) if line < STEPS else read(own_near_ref, 2 * STEPS - 1 - line)

    force = start(force_of)
    read = start(state_of)
    for step in range(1, STEPS):
        last = 2 * STEPS - 1 - step
        for line in range(step, last + 1):
            new = advance(read(line - 1), read(line), read(line + 1), force(line))
            levels[step - 1][line - step] = new
            for edge_ref, at in ((cross_edge_ref, line - step), (near_edge_ref, last - line)):
                if at < 2:
                    edge_ref[2 * (step - 1) + at] = new
        read = lambda line, step=step: levels[step - 1][line - step]


def border_lines(own_ref, got_ref, edge_ref, levels, kept, put):
    def start(read):
        return lambda at: read(own_ref, at) if at >= 0 else read(got_ref, -1 - at)

    force = start(force_of)
    read = start(state_of)
    for step in range(1, STEPS + 1):
        first = step - STEPS
        for at in range(first, first + STEPS):
            new = advance(read(at - 1), read(at), read(at + 1), force(at))
            if at < 0 and kept is not None:
                new = new * kept
            if step == STEPS:
                put(at, new)
            else:
                levels[step - 1][at - first] = new
        if step < STEPS:

            def read(at, step=step, first=first):
                if at < step:
                    return levels[step - 1][at - first]
                return edge_ref[2 * (step - 1) + at - step]


def near_kernel(own_ref, got_ref, edge_ref, done_ref, *levels):
    def put(at, value):
        done_ref[at] = value

    border_lines(own_ref, got_ref, edge_ref, levels, None, put)


def cross_kernel(last, strip_ref, columns_ref, done_ref, own_ref, got_ref, edge_ref, out_ref, *levels):
    strip = strip_ref[0]
    odd = lax.rem(strip, 2)
    leader = leader_of(strip)
    for at in range(STEPS):
        put_line(out_ref, odd, leader, 2 * STEPS - 1 - at, done_ref[at])
    kept = jnp.where(jnp.logical_or(strip == 0, strip == last), 0.0, 1.0)
    put = lambda at, value: put_line(out_ref, odd, leader, at, value)
    border_lines(own_ref, got_ref, edge_ref, levels, kept, put)


NN = (((1,), (0,)), ((), ()))
NT = (((1,), (1,)), ((), ()))


def halves(x):
    high = x.astype(jnp.bfloat16)
    return high, (x - high.astype(jnp.float32)).astype(jnp.bfloat16)


def dot(a, b, dims=NN):
    return lax.dot_general(a, b, dims, preferred_element_type=jnp.float32)


def across(parts):
    high, low = parts
    return jnp.concatenate([high, low, high], axis=1)


def down(parts):
    high, low = parts
    return jnp.concatenate([high, high, low], axis=0)


def stack(*parts):
    return tuple(jnp.concatenate(p, axis=0) for p in zip(*parts))


def product(a, b):
    return dot(across(a), down(b))


def analysis_kernel(columns_ref, block_ref, out_ref):
    chunks, per, _ = block_ref.shape
    members = chunks * per
    slots = columns_ref.shape[0]
    regions = block_ref.shape[2] // REGION_VALUES
    top = members - 1.0
    columns = columns_ref[...]
    eye = (lax.broadcasted_iota(jnp.int32, (slots, slots), 0) == lax.broadcasted_iota(jnp.int32, (slots, slots), 1)).astype(jnp.float32)
    cell = lax.broadcasted_iota(jnp.int32, (slots, REGION_VALUES), 1).astype(jnp.float32)

    def begin(r):
        cells = slice(r * REGION_VALUES, (r + 1) * REGION_VALUES)
        block = block_ref[:, :, cells].reshape(members, REGION_VALUES)
        index, root, value = (columns[:, 4 * r + i : 4 * r + i + 1] for i in range(3))
        mean = jnp.sum(block, axis=0, keepdims=True) * (1.0 / members)
        spread = block - mean
        sh, sl = halves(spread)
        chosen = cell == index
        onehot = chosen.astype(jnp.bfloat16)
        observed = dot(onehot, sh, NT) + dot(onehot, sl, NT)
        obs_mean = jnp.sum(jnp.where(chosen, mean, 0.0), axis=1, keepdims=True)
        scaled = observed * root
        misfit = root * (value - obs_mean)
        gh, gl = halves(scaled)
        small = dot(jnp.concatenate([gh, gl, gh], axis=1), jnp.concatenate([gh, gh, gl], axis=1), NT)
        carried = product((gh, gl), (sh, sl))
        norm = top + jnp.sqrt(jnp.sum(small * small, keepdims=True))
        inverse = 1.0 / norm
        return dict(mean=mean, scaled=scaled, misfit=misfit, carried=carried, norm=norm, inverse=inverse, small=small)

    def iterate(s):
        inverse = s["inverse"]
        left = (top * inverse) * eye + s["small"] * inverse
        left_zero = top * inverse
        fix = 1.5 * eye - 0.5 * left
        fix_zero = 1.5 - 0.5 * left_zero
        f = halves(fix)
        square = product(f, f)
        yield 2
        mixed = square - (0.5 * left_zero) * (fix + fix_zero * eye)
        left_rest = inverse * mixed
        left = product(halves(left), halves(square))
        yield 2
        right, right_zero, rest = fix, fix_zero, (-0.5 * inverse) * eye
        left_zero = left_zero * fix_zero * fix_zero
        for repeat in range(1, NS_ITERS):
            fix = 1.5 * eye - 0.5 * left
            fix_zero = 1.5 - 0.5 * left_zero
            f = halves(fix)
            last = repeat == NS_ITERS - 1
            rows = [halves(right)] if last else [f, halves(right), halves(left_rest)]
            if repeat > 1: rows.append(halves(rest))
            got = product(stack(*rows), f)
            got = [got[i * slots : (i + 1) * slots] for i in range(len(rows))]
            yield 2
            new_rest = (got[-1] if repeat > 1 else (-0.5 * inverse) * fix) - (0.5 * right_zero) * left_rest
            if not last:
                square, right, rest_fix = got[:3]
                both = product(stack(halves(left), halves(left_rest)), halves(square))
                left = both[:slots]
                left_rest = both[slots:] - (0.5 * left_zero) * (rest_fix + fix_zero * left_rest)
                left_zero = left_zero * fix_zero * fix_zero
                yield 2
            else:
                right = got[0]
            rest = new_rest
            right_zero = right_zero * fix_zero
        s.update(right=right, right_zero=right_zero, rest=rest)

    def finish(r, s):
        cells = slice(r * REGION_VALUES, (r + 1) * REGION_VALUES)
        right, carried = s["right"], s["carried"]
        along = jnp.sum(right * s["misfit"], axis=0, keepdims=True)
        twice = jnp.sum(right * along, axis=1, keepdims=True)
        moved = jnp.sum(twice * carried, axis=0, keepdims=True) * s["inverse"]
        pushed = product(halves(s["rest"]), halves(carried))
        gain = math.sqrt(top) * lax.rsqrt(s["norm"])
        update = product(halves(s["scaled"].T * gain), halves(pushed))
        block = block_ref[:, :, cells].reshape(members, REGION_VALUES)
        keep = gain * s["right_zero"]
        result = keep * block + (s["mean"] * (1.0 - keep) + moved) + update
        out_ref[:, :, cells] = result.reshape(chunks, per, REGION_VALUES)

    states = [begin(r) for r in range(regions)]
    runs = [iterate(s) for s in states]
    while runs:
        runs = [run for run in runs if next(run, 0)]
    for r in range(regions):
        finish(r, states[r])


def unpack_kernel(strip_ref, block_ref, out_ref):
    leader = leader_of(strip_ref[0])
    rows = out_ref.shape[1]
    parts = block_ref.shape[0] // rows
    width = block_ref.shape[2]
    for row in range(rows):
        for part in range(parts):
            out_ref[:, row, part * width : (part + 1) * width] = block_ref[rank_of(row * parts + part, leader, block_ref.shape[0])]


def local(ensemble, forcing, obs_index, obs_count, obs_value, obs_precision):
    per, rows, lon = ensemble.shape
    strips = lax.axis_size("strip")
    strip = lax.axis_index("strip").astype(jnp.int32).reshape(1)
    regions, slots = obs_index.shape
    message = jax.ShapeDtypeStruct((2 * STEPS + 1, per, lon // 2), jnp.float32)

    cross, near = pl.pallas_call(
        pack_kernel,
        out_shape=(message, message),
        in_specs=[SMEM, ANY, ANY],
        out_specs=(VMEM, VMEM),
        scratch_shapes=[
            pltpu.VMEM((2, per, rows, lon // 2), jnp.float32),
            pltpu.VMEM((rows, lon), jnp.float32),
            pltpu.SemaphoreType.DMA((3,)),
        ],
        compiler_params=params(),
        name="pack",
    )(strip, *(pltpu.with_memory_space_constraint(x, pltpu.HBM) for x in (ensemble, forcing)))
    span = [(i, i + 1) for i in range(1, strips - 1, 2)]
    span = span + [(b, a) for a, b in span]
    swap = [(i, i ^ 1) for i in range(strips)]
    got_cross = lax.ppermute(cross, "strip", span)
    got_near = lax.ppermute(near, "strip", swap)

    def line_slabs(count):
        return pltpu.VMEM((count, per, lon), jnp.float32)

    edges = jax.ShapeDtypeStruct((2 * (STEPS - 1), per, lon), jnp.float32)
    border_levels = [line_slabs(STEPS) for _ in range(1, STEPS)]
    columns, cross_edge, near_edge = pl.pallas_call(
        own_kernel,
        out_shape=(jax.ShapeDtypeStruct((slots, 4 * regions), jnp.float32), edges, edges),
        in_specs=[SMEM] + [VMEM] * 5,
        out_specs=(VMEM,) * 3,
        scratch_shapes=[line_slabs(2 * STEPS - 2 * step) for step in range(1, STEPS)],
        compiler_params=params(),
        cost_estimate=pl.CostEstimate(flops=10**8, bytes_accessed=4096, transcendentals=0),
        name="forecast_own",
    )(obs_count, obs_index, obs_value, obs_precision, cross, near)
    chunks = lax.axis_size("mem")
    width = rows * lon // chunks
    full = jax.ShapeDtypeStruct((chunks, per, width), jnp.float32)

    done = pl.pallas_call(
        near_kernel,
        out_shape=jax.ShapeDtypeStruct((STEPS, per, lon), jnp.float32),
        in_specs=[VMEM] * 3,
        out_specs=VMEM,
        scratch_shapes=border_levels,
        compiler_params=params(),
        cost_estimate=pl.CostEstimate(flops=10**8, bytes_accessed=4096, transcendentals=0),
        name="forecast_near",
    )(near, got_near, near_edge)
    sent = pl.pallas_call(
        functools.partial(cross_kernel, strips - 1),
        out_shape=full,
        in_specs=[SMEM, ANY] + [VMEM] * 4,
        out_specs=VMEM,
        scratch_shapes=border_levels,
        compiler_params=params(),
        name="forecast_cross",
    )(strip, columns, done, cross, got_cross, cross_edge)
    groups = [
        [i * chunks + (leader_of(i) + rank) % chunks for rank in range(chunks)] for i in range(strips)
    ]

    def exchange(x):
        return lax.all_to_all(x, ("strip", "mem"), split_axis=0, concat_axis=0, axis_index_groups=groups, tiled=True)

    regional = exchange(sent)
    analysed = pl.pallas_call(
        analysis_kernel,
        out_shape=jax.ShapeDtypeStruct((chunks, per, width), jnp.float32),
        in_specs=[VMEM] * 2,
        out_specs=VMEM,
        compiler_params=params(),
        name="analysis",
    )(columns, regional)
    back = exchange(analysed)
    return pl.pallas_call(
        unpack_kernel,
        out_shape=jax.ShapeDtypeStruct((per, rows, lon), jnp.float32),
        in_specs=[SMEM, VMEM],
        out_specs=VMEM,
        compiler_params=params(),
        name="unpack",
    )(strip, back)


def solution(mesh):
    placed = (
        P("mem", "strip", None),
        P("strip", None),
        P(("strip", "mem"), None),
        P(("strip", "mem")),
        P(("strip", "mem"), None),
        P(("strip", "mem"), None),
    )
    return jax.shard_map(local, mesh=mesh, in_specs=placed, out_specs=P("mem", "strip", None), check_vma=False)
```
